32 devices in a mesh: robot: 8 (over y, x, core), seed: 4 (over z).
Axes of the slice: x: 2, y: 2, z: 4, core: 2. Of those that a mesh axis runs over, the one named last changes fastest.
Arguments:
- centres: float32 [16, 3, 52, 1024], P('robot', None, None, 'seed'), may hold values from -36 to 36
- sphere_radius: float32 [16, 52], P('robot'), may hold values from 0.2 to 0.8
- counts: int32 [16], P('robot'), may hold values from 26 to 52
- adjacency: int32 [16, 16], P('robot'), may hold values from 0 to 1, as said below
Outputs:
- collision_cost: float32 [16, 1024], P('robot', 'seed')
- blended_path: float32 [16, 3, 52, 32], P('robot')
The draws below stay inside these ranges and needn't reach their ends.
Inputs may be any that keep to these rules, and one draw needn't show every extreme that they name: `adjacency`: symmetric, with zeros on the diagonal.
All inputs are finite; a program needn't handle non-finite values.
Results may differ from the reference program's by a relative error of at most 0.0003.
Values sent between devices are 32-bit elements; how exact they have to be, the bound alone decides.
No kernel may reach another device: no remote copies, remote signals or barrier semaphores. Data moves between devices by JAX's collectives and lax.ppermute only.
A program may use at most 64 MiB of HBM per device.

```python
import math
import jax
import jax.numpy as jnp
import numpy as np
from jax import lax

P_SIZE = 52
W = 32
ROBOTS = 16
SEEDS = 32


grid_columns = 4


spacing = 1.8


def cell_slots(key):
    return jax.random.permutation(jax.random.fold_in(key, 7), ROBOTS).astype(jnp.int32)


def draw_adjacency(key, part):
    slot = cell_slots(key)
    grid_row = slot // grid_columns
    grid_col = slot % grid_columns
    row_gap = jnp.abs(grid_row[:, None] - grid_row[None, :])
    col_gap = jnp.abs(grid_col[:, None] - grid_col[None, :])
    linked = (row_gap <= 1) & (col_gap <= 1) & (slot[:, None] != slot[None, :])
    return linked.astype(jnp.int32)


def draw_centres(key, part):
    slot = cell_slots(key)
    grid_row = (slot // grid_columns).astype(jnp.float32)
    grid_col = (slot % grid_columns).astype(jnp.float32)
    row_total = ROBOTS // grid_columns
    base_x = spacing * (grid_col - 0.5 * (grid_columns - 1))
    base_y = spacing * (grid_row - 0.5 * (row_total - 1))
    base = jnp.stack([base_x, base_y, jnp.zeros_like(base_x)], axis=1)
    sphere_order = jnp.arange(P_SIZE, dtype=jnp.int32)
    side = jnp.where(sphere_order < P_SIZE // 2, -0.6, 0.6).astype(jnp.float32)
    lobes = jnp.stack([jnp.zeros_like(side), side, jnp.full_like(side, 0.8)], axis=0)
    arm_key = jax.random.fold_in(key, 31)
    shift_key = jax.random.fold_in(key, 37)
    scale_key = jax.random.fold_in(key, 41)
    step_key = jax.random.fold_in(key, 43)
    step_scale = jnp.exp(jax.random.uniform(scale_key, (ROBOTS, 1, P_SIZE, 1, 1), jnp.float32, jnp.log(0.04), jnp.log(0.15)))
    arm = 0.5 * jnp.clip(jax.random.normal(arm_key, (ROBOTS, 3, P_SIZE), jnp.float32), -4.0, 4.0)
    shift = 0.5 * jnp.clip(jax.random.normal(shift_key, (ROBOTS, 3, SEEDS), jnp.float32), -3.0, 3.0)
    steps = step_scale * jnp.clip(jax.random.normal(step_key, (ROBOTS, 3, P_SIZE, SEEDS, W - 1), jnp.float32), -3.0, 3.0)
    walk = jnp.concatenate([jnp.zeros((ROBOTS, 3, P_SIZE, SEEDS, 1), jnp.float32), jnp.cumsum(steps, axis=4)], axis=4)
    centre = base[:, :, None, None, None] + lobes[None, :, :, None, None] + arm[:, :, :, None, None]
    centre = centre + shift[:, :, None, :, None] + walk
    return centre.reshape(ROBOTS, 3, P_SIZE, SEEDS * W)


def with_ends(result, own_key, smallest, high):
    longest = result.shape.index(max(result.shape))
    spots = []
    for shift in (0, 1):
        where = [jax.random.randint(jax.random.fold_in(own_key, axis), (), 0, length) for axis, length in enumerate(result.shape)]
        where[longest] = (where[longest] + shift) % result.shape[longest]
        spots.append(tuple(where))
    return result.at[spots[0]].set(smallest).at[spots[1]].set(high)


def shard_levels(stream_key, extent, shards, low, top_value):
    level, own = 1.0, jax.random.fold_in(stream_key, 6)
    for position, shards_of in shards:
        steps = jnp.exp(jax.random.uniform(jax.random.fold_in(own, position), (shards_of,), jnp.float32, low / len(shards), top_value / len(shards)))
        level = level * jnp.repeat(steps, extent[position] // shards_of).reshape([-1 if axis == position else 1 for axis in range(len(extent))])
    return level


def setup_inputs(seed: int = 0) -> dict:
    seeds = jax.random.split(jax.random.key(seed), 5)
    centres = draw_centres(jax.random.fold_in(seeds[4], 71), 0)
    sphere_radius = jnp.clip(jnp.exp(math.log(0.8) - 1.3862944 * jax.random.uniform(seeds[1], (ROBOTS, P_SIZE), jnp.float32) ** shard_levels(seeds[1], (ROBOTS, P_SIZE), ((0, 8),), -0.2, 0.2)), 0.2, 0.8)
    counts = with_ends(jax.random.randint(seeds[2], (ROBOTS,), P_SIZE // 2, P_SIZE + 1), jax.random.fold_in(seeds[2], 1), P_SIZE // 2, P_SIZE).astype(jnp.int32)
    adjacency = draw_adjacency(jax.random.fold_in(seeds[4], 71), 0)
    return {"centres": centres, "sphere_radius": sphere_radius, "counts": counts, "adjacency": adjacency}


lane_width = 128

def swept_blocks(centres, sphere_radius):
    robots_here, _, spheres, columns = centres.shape
    shaped = centres.reshape(robots_here, 3, spheres, columns // W, W)
    ahead_point = jnp.concatenate([shaped[..., 1:], shaped[..., -1:]], axis=4)
    middle = 0.5 * (shaped + ahead_point)
    step_length = jnp.sqrt(lax.optimization_barrier(jnp.sum((ahead_point - shaped) ** 2, axis=1)) + 1e-06)
    swept_radius = sphere_radius[:, :, None, None] + 0.5 * step_length
    swept_block = jnp.concatenate([middle, swept_radius[:, None]], axis=1)
    return swept_block.reshape(robots_here, 4, spheres, columns)

def active_spheres(counts, spheres):
    return (jnp.arange(spheres, dtype=jnp.int32)[None, :] < counts[:, None]).astype(jnp.float32)

def pair_cost(first_block, first_active, second_block, second_active, sphere_mask):
    spheres = first_block.shape[1]
    columns = first_block.shape[2]
    weights = first_active[:, None] * second_active[None, :] * sphere_mask

    def tile_cost(tile_index):
        offset = tile_index * lane_width
        first_tile = lax.dynamic_slice_in_dim(first_block, offset, lane_width, 2)
        second_tile = lax.dynamic_slice_in_dim(second_block, offset, lane_width, 2)
        distance = jnp.zeros((spheres, spheres, lane_width), jnp.float32)
        for axis_index in range(3):
            gap = first_tile[axis_index][:, None, :] - second_tile[axis_index][None, :, :]
            distance = distance + gap * gap
        spread = first_tile[3][:, None, :] + second_tile[3][None, :, :]
        return lax.optimization_barrier(jnp.sum(weights[:, :, None] * jnp.exp(-distance / (spread * spread)), axis=(0, 1)))
    tiles = lax.map(tile_cost, jnp.arange(columns // lane_width, dtype=jnp.int32))
    return tiles.reshape(columns) / (spheres * spheres)

def self_costs(own_blocks, own_active):
    spheres = own_blocks.shape[2]
    order = jnp.arange(spheres, dtype=jnp.int32)
    apart = (order[None, :] >= order[:, None] + 2).astype(jnp.float32)

    def single(robot_row):
        return pair_cost(own_blocks[robot_row], own_active[robot_row], own_blocks[robot_row], own_active[robot_row], apart)
    return lax.map(single, jnp.arange(own_blocks.shape[0], dtype=jnp.int32))

def seed_weights(centres, robot_cost):
    robots_here, _, spheres, columns = centres.shape
    seed_count = columns // W
    seed_cost = lax.optimization_barrier(jnp.sum(robot_cost.reshape(robots_here, seed_count, W), axis=2))
    weight = 1.0 / (1.0 + seed_cost)
    shaped = centres.reshape(robots_here, 3, spheres, seed_count, W)
    weighted = lax.optimization_barrier(jnp.sum(shaped * weight[:, None, None, :, None], axis=3))
    return (weighted, lax.optimization_barrier(jnp.sum(weight, axis=1)))

def reference(centres, sphere_radius, counts, adjacency):
    blocks = swept_blocks(centres, sphere_radius)
    spheres = blocks.shape[2]
    columns = blocks.shape[3]
    active = active_spheres(counts, spheres)
    full_mask = jnp.ones((spheres, spheres), jnp.float32)
    start_cost = self_costs(blocks, active)
    firsts, seconds = np.triu_indices(ROBOTS, 1)
    pair_list = jnp.asarray(np.stack([firsts, seconds], axis=1), dtype=jnp.int32)

    def add_pair(totals_now, pair_row):
        first_row = pair_row[0]
        second_row = pair_row[1]
        pair_term = lax.cond(adjacency[first_row, second_row] != 0, lambda: pair_cost(blocks[first_row], active[first_row], blocks[second_row], active[second_row], full_mask), lambda: jnp.zeros((columns,), jnp.float32))
        return (totals_now.at[first_row].add(pair_term).at[second_row].add(pair_term), None)
    robot_cost, _ = lax.scan(add_pair, start_cost, pair_list)
    weighted, totals = seed_weights(centres, robot_cost)
    return (robot_cost, weighted / totals[:, None, None, None])
```

```python
import functools
import math

import jax
import jax.numpy as jnp
from jax import lax
from jax.experimental import pallas as pl
from jax.experimental.pallas import tpu as pltpu
from jax.sharding import PartitionSpec as P

W = 32
LANES = 128
SUB = 8
SCALE = math.sqrt(math.log2(math.e))
FAR = 1e15
VMEM = pl.BlockSpec(memory_space=pltpu.VMEM)
SMEM = pl.BlockSpec(memory_space=pltpu.SMEM)


def round_up(value, step):
    return -(-value // step) * step


class Plan:
    def __init__(self, group, robots_here, spheres, columns):
        self.group = group
        self.here = robots_here
        self.spheres = spheres
        self.columns = columns
        self.width = columns // group
        self.lane_groups = LANES // self.width
        self.rows = -(-spheres // self.lane_groups)
        self.padded = self.rows * self.lane_groups
        self.block_rows = round_up(self.rows, SUB)
        self.slots = group * robots_here
        self.halves = -(-self.slots // 16)
        self.data_rows = robots_here * 4 * self.rows
        self.chunk_rows = round_up(self.data_rows + 1, SUB)
        self.tiles = columns // LANES


def iota(shape, axis):
    return lax.broadcasted_iota(jnp.int32, shape, axis)


def pack_kernel(plan, counts, radius, adjacency, centres, *refs):
    outs, raw, swept = refs[:-2], refs[-2], refs[-1]
    me = lax.axis_index("robot")
    n, g, rows, width = plan.spheres, plan.lane_groups, plan.rows, plan.width
    last = iota((n, LANES), 1) % W == W - 1
    order = iota((n, LANES), 0)
    diagonal = iota((n, n), 0) == iota((n, n), 1)
    for l in range(plan.here):
        column = jnp.sum(jnp.where(diagonal, radius[l : l + 1, :], 0.0), axis=1, keepdims=True)
        robot = me * plan.here + l
        off = FAR * (1 + order + plan.padded * robot).astype(jnp.float32)
        for t in range(plan.tiles):
            squares = jnp.zeros((n, LANES), jnp.float32)
            for c in range(3):
                x = centres[l, c, :, t * LANES : (t + 1) * LANES]
                raw[t, l * 3 + c] = x
                ahead = jnp.where(last, x, pltpu.roll(x, LANES - 1, 1))
                middle = (0.5 * SCALE) * (x + ahead)
                if c == 0:
                    middle = jnp.where(order < counts[l], middle, off)
                swept[t, l * 4 + c, 0:n, :] = middle
                squares = squares + (ahead - x) * (ahead - x)
            swept[t, l * 4 + 3, 0:n, :] = column + 0.5 * jnp.sqrt(squares + 1e-06)
            if plan.padded > n:
                spare = plan.padded - n
                index = n + iota((spare, LANES), 0) + plan.padded * robot
                swept[t, l * 4, n:, :] = FAR * (1 + index).astype(jnp.float32)
                for c in range(1, 4):
                    swept[t, l * 4 + c, n:, :] = jnp.ones((spare, LANES), jnp.float32)
    lane = iota((1, LANES), 1)
    head = jnp.zeros((1, LANES), jnp.float32)
    links = iota((1, plan.slots), 1)
    for l in range(plan.here):
        at = l * (1 + plan.halves)
        head = jnp.where(lane == at, counts[l].astype(jnp.float32), head)
        for h in range(plan.halves):
            bits = jnp.where(
                (adjacency[l : l + 1, :] != 0) & (links // 16 == h), 1 << (links % 16), 0
            ).astype(jnp.float32)
            head = jnp.where(lane == at + 1 + h, jnp.sum(bits, axis=1, keepdims=True), head)
    lane_group = iota((rows, LANES), 1) // width
    for k in range(plan.group):
        dest = me ^ k
        tile = dest // g
        spot = dest % g
        for rc in range(plan.here * 4):
            y = jnp.zeros((rows, LANES), jnp.float32)
            for j in range(g):
                x = swept[tile, rc, pl.ds(j, rows, stride=g), :]
                x = pltpu.roll(x, ((j + g - spot) % g) * width, 1)
                y = jnp.where(lane_group == j, x, y)
            outs[k][rc * rows : (rc + 1) * rows, :] = y
        outs[k][plan.data_rows : plan.data_rows + 1, :] = head


def pack(plan, counts, radius, adjacency, centres):
    chunk = jax.ShapeDtypeStruct((plan.chunk_rows, LANES), jnp.float32)
    return pl.pallas_call(
        functools.partial(pack_kernel, plan),
        out_shape=[chunk] * plan.group
        + [jax.ShapeDtypeStruct((plan.tiles, plan.here * 3, plan.spheres, LANES), jnp.float32)],
        in_specs=[SMEM, VMEM, VMEM, VMEM],
        out_specs=[VMEM] * (plan.group + 1),
        scratch_shapes=[pltpu.VMEM((plan.tiles, plan.here * 4, plan.padded, LANES), jnp.float32)],
        name="pack",
    )(counts, radius, adjacency, centres)


def term(first, second):
    gap = first[0] - second[0]
    square = gap * gap
    for c in (1, 2):
        gap = first[c] - second[c]
        square = square + gap * gap
    inverse = 1.0 / (first[3] + second[3])
    return jnp.exp2(-(square * (inverse * inverse)))


def cost_kernel(plan, *refs):
    chunks = refs[: plan.group]
    out, blocks, totals, heads, sem = refs[plan.group :]
    me = lax.axis_index("robot")
    g, rows, width, here = plan.lane_groups, plan.rows, plan.width, plan.here
    parts = plan.block_rows // SUB
    copies = [
        pltpu.make_async_copy(
            chunks[k].at[pl.ds(plan.data_rows, 1)], heads.at[pl.ds(k, 1)], sem.at[k]
        )
        for k in range(plan.group)
    ]
    for copy in copies:
        copy.start()
    spare = plan.block_rows - rows
    for k in range(plan.group):
        for l in range(here):
            for c in range(4):
                x = chunks[k][(l * 4 + c) * rows : (l * 4 + c + 1) * rows, :]
                for m in range(g):
                    blocks[k * here + l, c, m, 0:rows, :] = pltpu.roll(x, m * width, 1) if m else x
                if spare:
                    fill = -FAR if c == 0 else 1.0
                    blocks[k * here + l, c, 0, rows:, :] = jnp.full((spare, LANES), fill, jnp.float32)
    totals[...] = jnp.zeros_like(totals)
    for copy in copies:
        copy.wait()

    def row(slot, m, r):
        return [blocks[slot, c, m, r : r + 1, :] for c in range(4)]

    def part(slot, i):
        return [blocks[slot, c, 0, i * SUB : (i + 1) * SUB, :] for c in range(4)]

    later = g * iota((SUB, LANES), 0) + iota((SUB, LANES), 1) // width

    @pl.loop(0, plan.slots)
    def _(u):
        total = jnp.zeros((SUB, LANES), jnp.float32)
        for i in range(parts):
            second = part(u, i)
            for m in range(g):
                ahead = later - (iota((SUB, LANES), 1) // width + g - m) % g + g * SUB * i
                for r in range(min(rows, (i + 1) * SUB)):
                    value = term(row(u, m, r), second)
                    if (r + 1) * g + 1 > g * SUB * i:
                        value = jnp.where(ahead >= g * r + 2, value, 0.0)
                    total = total + value
        totals[u] = totals[u] + total
        links = [
            heads[u // here, (u % here) * (1 + plan.halves) + 1 + h].astype(jnp.int32)
            for h in range(plan.halves)
        ]

        @pl.loop(u + 1, plan.slots)
        def _(v):
            robot = v ^ (me * here)
            mask = links[0]
            for h in range(1, plan.halves):
                mask = jnp.where(robot // 16 == h, links[h], mask)

            @pl.when((mask >> (robot % 16)) & 1 == 1)
            def _():
                total = jnp.zeros((SUB, LANES), jnp.float32)
                for i in range(parts):
                    second = part(v, i)
                    for m in range(g):
                        for r in range(rows):
                            total = total + term(row(u, m, r), second)
                totals[u] = totals[u] + total
                totals[v] = totals[v] + total

    spot = iota((1, LANES), 1) // width == me % g
    for k in range(plan.group):
        for l in range(here):
            value = jnp.sum(totals[k * here + l], axis=0, keepdims=True)
            shift = width
            while shift < LANES:
                value = value + pltpu.roll(value, shift, 1)
                shift *= 2
            value = jnp.where(spot, value, 0.0) / (plan.spheres * plan.spheres)
            out[pl.ds((me ^ k) * here + l, 1), :] = value


def cost(plan, chunks):
    slots, g = plan.slots, plan.lane_groups
    return pl.pallas_call(
        functools.partial(cost_kernel, plan),
        out_shape=jax.ShapeDtypeStruct((plan.slots, LANES), jnp.float32),
        in_specs=[VMEM] * plan.group,
        out_specs=VMEM,
        scratch_shapes=[
            pltpu.VMEM((slots, 4, g, plan.block_rows, LANES), jnp.float32),
            pltpu.VMEM((slots, SUB, LANES), jnp.float32),
            pltpu.SMEM((plan.group, LANES), jnp.float32),
            pltpu.SemaphoreType.DMA((plan.group,)),
        ],
        name="cost",
    )(*chunks)


def blend_kernel(plan, seeds_here, costs, raw, cost_out, sums):
    n, here, g = plan.spheres, plan.here, plan.lane_groups
    n_rows = n // 4
    seed_of = iota((seeds_here, LANES), 1) // W
    seed = iota((seeds_here, LANES), 0)
    fold = iota((n_rows, LANES), 1) // W
    per_tile = LANES // W
    for l in range(here):
        lines = []
        seed_cost = jnp.zeros((seeds_here, 1), jnp.float32)
        for t in range(plan.tiles):
            line = costs[t * g * here + l : t * g * here + l + 1, :]
            for d in range(t * g + 1, (t + 1) * g):
                line = line + costs[d * here + l : d * here + l + 1, :]
            cost_out[l : l + 1, t * LANES : (t + 1) * LANES] = line
            lines.append(line)
            mine = seed_of + t * per_tile == seed
            seed_cost = seed_cost + jnp.sum(jnp.where(mine, line, 0.0), axis=1, keepdims=True)
        weight = 1.0 / (1.0 + seed_cost)
        spread = []
        for t in range(plan.tiles):
            mine = seed_of + t * per_tile == seed
            spread.append(jnp.sum(jnp.where(mine, weight, 0.0), axis=0, keepdims=True))
        total = jnp.sum(weight, axis=0, keepdims=True)
        sums[here * 3 * n_rows + l : here * 3 * n_rows + l + 1, :] = jnp.broadcast_to(total, (1, LANES))
        for c in range(3):
            pieces = []
            for j in range(4):
                x = jnp.zeros((n_rows, LANES), jnp.float32)
                for t in range(plan.tiles):
                    part = raw[t, l * 3 + c, pl.ds(j, n_rows, stride=4), :]
                    x = x + part * spread[t]
                pieces.append(x)
            y = jnp.zeros((n_rows, LANES), jnp.float32)
            for turn in range(4):
                z = pieces[0]
                for j in range(4):
                    z = jnp.where(fold == (j - turn) % 4, pieces[j], z)
                y = y + (pltpu.roll(z, turn * W, 1) if turn else z)
            at = (l * 3 + c) * n_rows
            sums[at : at + n_rows, :] = y


def blend(plan, costs, raw):
    seeds_here = plan.columns // W
    rows = round_up(plan.here * (3 * plan.spheres // 4 + 1), SUB)
    return pl.pallas_call(
        functools.partial(blend_kernel, plan, seeds_here),
        out_shape=[
            jax.ShapeDtypeStruct((plan.here, plan.columns), jnp.float32),
            jax.ShapeDtypeStruct((rows, LANES), jnp.float32),
        ],
        in_specs=[VMEM, VMEM],
        out_specs=[VMEM, VMEM],
        name="blend",
    )(costs, raw)


def finish_kernel(plan, *refs):
    parts, out, wide = refs[:-2], refs[-2], refs[-1]
    n_rows = plan.spheres // 4
    for l in range(plan.here):
        at = plan.here * 3 * n_rows + l
        total = parts[0][at : at + 1, :]
        for p in parts[1:]:
            total = total + p[at : at + 1, :]
        inverse = 1.0 / total
        for c in range(3):
            at = (l * 3 + c) * n_rows
            y = parts[0][at : at + n_rows, :]
            for p in parts[1:]:
                y = y + p[at : at + n_rows, :]
            y = y * inverse
            for j in range(4):
                z = pltpu.roll(y, (LANES - j * W) % LANES, 1) if j else y
                wide[pl.ds(j, n_rows, stride=4), :] = z
            out[l, c] = wide[:, :W]


def finish(plan, parts):
    return pl.pallas_call(
        functools.partial(finish_kernel, plan),
        out_shape=jax.ShapeDtypeStruct((plan.here, 3, plan.spheres, W), jnp.float32),
        in_specs=[VMEM] * len(parts),
        out_specs=VMEM,
        scratch_shapes=[pltpu.VMEM((plan.spheres, LANES), jnp.float32)],
        name="finish",
    )(*parts)


def exchanged(block, axis, k):
    size = lax.axis_size(axis)
    return lax.ppermute(block, axis, [(i, i ^ k) for i in range(size)])


def local(centres, sphere_radius, counts, adjacency):
    here, _, spheres, columns = centres.shape
    plan = Plan(lax.axis_size("robot"), here, spheres, columns)
    *chunks, raw = pack(plan, counts, sphere_radius, adjacency, centres)
    chunks = [chunks[0]] + [exchanged(chunks[k], "robot", k) for k in range(1, plan.group)]
    costs = cost(plan, chunks)
    costs = lax.all_to_all(costs, "robot", 0, 0, tiled=True)
    robot_cost, sums = blend(plan, costs, raw)
    parts = [sums] + [exchanged(sums, "seed", k) for k in range(1, lax.axis_size("seed"))]
    return robot_cost, finish(plan, parts)


def solution(mesh):
    return jax.shard_map(
        local,
        mesh=mesh,
        in_specs=(P("robot", None, None, "seed"), P("robot", None), P("robot"), P("robot", None)),
        out_specs=(P("robot", "seed"), P("robot", None, None, None)),
        check_vma=False,
    )
```

```python
import functools
import math

import jax
import jax.numpy as jnp
from jax import lax
from jax.experimental import pallas as pl
from jax.experimental.pallas import tpu as pltpu
from jax.sharding import PartitionSpec as P

W = 32
LANES = 128
SUB = 8
SCALE = math.sqrt(math.log2(math.e))
FAR = 1e15
VMEM = pl.BlockSpec(memory_space=pltpu.VMEM)
SMEM = pl.BlockSpec(memory_space=pltpu.SMEM)
PARAMS = pltpu.CompilerParams(vmem_limit_bytes=16 * 1024 * 1024)


def round_up(value, step):
    return -(-value // step) * step


class Plan:
    def __init__(self, group, robots_here, spheres, columns):
        self.group = group
        self.here = robots_here
        self.spheres = spheres
        self.columns = columns
        self.width = columns // group
        self.lane_groups = LANES // self.width
        self.rows = -(-spheres // self.lane_groups)
        self.padded = self.rows * self.lane_groups
        self.block_rows = round_up(self.rows, SUB)
        self.slots = group * robots_here
        self.halves = -(-self.slots // 16)
        self.data_rows = robots_here * 4 * self.rows
        self.chunk_rows = round_up(self.data_rows + 1, SUB)
        self.tiles = columns // LANES


def iota(shape, axis):
    return lax.broadcasted_iota(jnp.int32, shape, axis)


def pack_kernel(plan, counts, radius, adjacency, centres, *refs):
    outs, raw, swept = refs[:-2], refs[-2], refs[-1]
    me = lax.axis_index("robot")
    n, g, rows, width = plan.spheres, plan.lane_groups, plan.rows, plan.width
    last = iota((n, LANES), 1) % W == W - 1
    order = iota((n, LANES), 0)
    diagonal = iota((n, n), 0) == iota((n, n), 1)
    for l in range(plan.here):
        column = jnp.sum(jnp.where(diagonal, radius[l : l + 1, :], 0.0), axis=1, keepdims=True)
        robot = me * plan.here + l
        off = FAR * (1 + order + plan.padded * robot).astype(jnp.float32)
        for t in range(plan.tiles):
            squares = jnp.zeros((n, LANES), jnp.float32)
            for c in range(3):
                at = (c * n * plan.tiles + t) * plan.here + l
                x = centres[pl.ds(at, n, stride=plan.tiles * plan.here), :]
                raw[t, l * 3 + c] = x
                ahead = jnp.where(last, x, pltpu.roll(x, LANES - 1, 1))
                middle = (0.5 * SCALE) * (x + ahead)
                if c == 0:
                    middle = jnp.where(order < counts[l], middle, off)
                swept[t, l * 4 + c, 0:n, :] = middle
                squares = squares + (ahead - x) * (ahead - x)
            swept[t, l * 4 + 3, 0:n, :] = column + 0.5 * jnp.sqrt(squares + 1e-06)
            if plan.padded > n:
                spare = plan.padded - n
                index = n + iota((spare, LANES), 0) + plan.padded * robot
                swept[t, l * 4, n:, :] = FAR * (1 + index).astype(jnp.float32)
                for c in range(1, 4):
                    swept[t, l * 4 + c, n:, :] = jnp.ones((spare, LANES), jnp.float32)
    lane = iota((1, LANES), 1)
    head = jnp.zeros((1, LANES), jnp.float32)
    links = iota((1, plan.slots), 1)
    for l in range(plan.here):
        at = l * (1 + plan.halves)
        head = jnp.where(lane == at, counts[l].astype(jnp.float32), head)
        for h in range(plan.halves):
            bits = jnp.where(
                (adjacency[l : l + 1, :] != 0) & (links // 16 == h), 1 << (links % 16), 0
            ).astype(jnp.float32)
            head = jnp.where(lane == at + 1 + h, jnp.sum(bits, axis=1, keepdims=True), head)
    lane_group = iota((rows, LANES), 1) // width
    for k in range(plan.group):
        dest = me ^ k
        tile = dest // g
        spot = dest % g
        for rc in range(plan.here * 4):
            y = jnp.zeros((rows, LANES), jnp.float32)
            for j in range(g):
                x = swept[tile, rc, pl.ds(j, rows, stride=g), :]
                x = pltpu.roll(x, ((j + g - spot) % g) * width, 1)
                y = jnp.where(lane_group == j, x, y)
            outs[k][rc * rows : (rc + 1) * rows, :] = y
        outs[k][plan.data_rows : plan.data_rows + 1, :] = head


def pack(plan, counts, radius, adjacency, centres):
    chunk = jax.ShapeDtypeStruct((plan.chunk_rows, LANES), jnp.float32)
    return pl.pallas_call(
        functools.partial(pack_kernel, plan),
        out_shape=[chunk] * plan.group
        + [jax.ShapeDtypeStruct((plan.tiles, plan.here * 3, plan.spheres, LANES), jnp.float32)],
        in_specs=[SMEM, VMEM, VMEM, VMEM],
        out_specs=[VMEM] * (plan.group + 1),
        scratch_shapes=[pltpu.VMEM((plan.tiles, plan.here * 4, plan.padded, LANES), jnp.float32)],
        compiler_params=PARAMS,
        name="pack",
    )(counts, radius, adjacency, centres)


def term(first, second):
    gap = first[0] - second[0]
    square = gap * gap
    for c in (1, 2):
        gap = first[c] - second[c]
        square = square + gap * gap
    inverse = 1.0 / (first[3] + second[3])
    return jnp.exp2(-(square * (inverse * inverse)))


def cost_kernel(plan, *refs):
    chunks = refs[: plan.group]
    out, blocks, totals, heads, sem = refs[plan.group :]
    me = lax.axis_index("robot")
    g, rows, width, here = plan.lane_groups, plan.rows, plan.width, plan.here
    parts = plan.block_rows // SUB
    copies = [
        pltpu.make_async_copy(
            chunks[k].at[pl.ds(plan.data_rows, 1)], heads.at[pl.ds(k, 1)], sem.at[k]
        )
        for k in range(plan.group)
    ]
    for copy in copies:
        copy.start()
    spare = plan.block_rows - rows
    for k in range(plan.group):
        for l in range(here):
            for c in range(4):
                x = chunks[k][(l * 4 + c) * rows : (l * 4 + c + 1) * rows, :]
                for m in range(g):
                    blocks[k * here + l, c, m, 0:rows, :] = pltpu.roll(x, m * width, 1) if m else x
                if spare:
                    fill = -FAR if c == 0 else 1.0
                    blocks[k * here + l, c, 0, rows:, :] = jnp.full((spare, LANES), fill, jnp.float32)
    totals[...] = jnp.zeros_like(totals)
    for copy in copies:
        copy.wait()

    def row(slot, m, r):
        return [blocks[slot, c, m, r : r + 1, :] for c in range(4)]

    def part(slot, i):
        return [blocks[slot, c, 0, i * SUB : (i + 1) * SUB, :] for c in range(4)]

    later = g * iota((SUB, LANES), 0) + iota((SUB, LANES), 1) // width

    @pl.loop(0, plan.slots)
    def _(u):
        total = jnp.zeros((SUB, LANES), jnp.float32)
        for i in range(parts):
            second = part(u, i)
            for m in range(g):
                ahead = later - (iota((SUB, LANES), 1) // width + g - m) % g + g * SUB * i
                for r in range(min(rows, (i + 1) * SUB)):
                    value = term(row(u, m, r), second)
                    if (r + 1) * g + 1 > g * SUB * i:
                        value = jnp.where(ahead >= g * r + 2, value, 0.0)
                    total = total + value
        totals[u] = totals[u] + total
        links = [
            heads[u // here, (u % here) * (1 + plan.halves) + 1 + h].astype(jnp.int32)
            for h in range(plan.halves)
        ]

        @pl.loop(u + 1, plan.slots)
        def _(v):
            robot = v ^ (me * here)
            mask = links[0]
            for h in range(1, plan.halves):
                mask = jnp.where(robot // 16 == h, links[h], mask)

            @pl.when((mask >> (robot % 16)) & 1 == 1)
            def _():
                total = jnp.zeros((SUB, LANES), jnp.float32)
                for i in range(parts):
                    second = part(v, i)
                    for m in range(g):
                        for r in range(rows):
                            total = total + term(row(u, m, r), second)
                totals[u] = totals[u] + total
                totals[v] = totals[v] + total

    spot = iota((1, LANES), 1) // width == me % g
    for k in range(plan.group):
        for l in range(here):
            value = jnp.sum(totals[k * here + l], axis=0, keepdims=True)
            shift = width
            while shift < LANES:
                value = value + pltpu.roll(value, shift, 1)
                shift *= 2
            value = jnp.where(spot, value, 0.0) / (plan.spheres * plan.spheres)
            out[pl.ds((me ^ k) * here + l, 1), :] = value


def cost(plan, chunks):
    slots, g = plan.slots, plan.lane_groups
    return pl.pallas_call(
        functools.partial(cost_kernel, plan),
        out_shape=jax.ShapeDtypeStruct((plan.slots, LANES), jnp.float32),
        in_specs=[VMEM] * plan.group,
        out_specs=VMEM,
        scratch_shapes=[
            pltpu.VMEM((slots, 4, g, plan.block_rows, LANES), jnp.float32),
            pltpu.VMEM((slots, SUB, LANES), jnp.float32),
            pltpu.SMEM((plan.group, LANES), jnp.float32),
            pltpu.SemaphoreType.DMA((plan.group,)),
        ],
        compiler_params=PARAMS,
        name="cost",
    )(*chunks)


def blend_kernel(plan, seeds_here, costs, raw, cost_out, sums):
    n, here, g = plan.spheres, plan.here, plan.lane_groups
    n_rows = n // 4
    seed_of = iota((seeds_here, LANES), 1) // W
    seed = iota((seeds_here, LANES), 0)
    fold = iota((n_rows, LANES), 1) // W
    per_tile = LANES // W
    for l in range(here):
        lines = []
        seed_cost = jnp.zeros((seeds_here, 1), jnp.float32)
        for t in range(plan.tiles):
            line = costs[t * g * here + l : t * g * here + l + 1, :]
            for d in range(t * g + 1, (t + 1) * g):
                line = line + costs[d * here + l : d * here + l + 1, :]
            cost_out[l : l + 1, t * LANES : (t + 1) * LANES] = line
            lines.append(line)
            mine = seed_of + t * per_tile == seed
            seed_cost = seed_cost + jnp.sum(jnp.where(mine, line, 0.0), axis=1, keepdims=True)
        weight = 1.0 / (1.0 + seed_cost)
        spread = []
        for t in range(plan.tiles):
            mine = seed_of + t * per_tile == seed
            spread.append(jnp.sum(jnp.where(mine, weight, 0.0), axis=0, keepdims=True))
        total = jnp.sum(weight, axis=0, keepdims=True)
        sums[here * 3 * n_rows + l : here * 3 * n_rows + l + 1, :] = jnp.broadcast_to(total, (1, LANES))
        for c in range(3):
            pieces = []
            for j in range(4):
                x = jnp.zeros((n_rows, LANES), jnp.float32)
                for t in range(plan.tiles):
                    part = raw[t, l * 3 + c, pl.ds(j, n_rows, stride=4), :]
                    x = x + part * spread[t]
                pieces.append(x)
            y = jnp.zeros((n_rows, LANES), jnp.float32)
            for turn in range(4):
                z = pieces[0]
                for j in range(4):
                    z = jnp.where(fold == (j - turn) % 4, pieces[j], z)
                y = y + (pltpu.roll(z, turn * W, 1) if turn else z)
            at = (l * 3 + c) * n_rows
            sums[at : at + n_rows, :] = y


def blend(plan, costs, raw):
    seeds_here = plan.columns // W
    rows = round_up(plan.here * (3 * plan.spheres // 4 + 1), SUB)
    return pl.pallas_call(
        functools.partial(blend_kernel, plan, seeds_here),
        out_shape=[
            jax.ShapeDtypeStruct((plan.here, plan.columns), jnp.float32),
            jax.ShapeDtypeStruct((rows, LANES), jnp.float32),
        ],
        in_specs=[VMEM, VMEM],
        out_specs=[VMEM, VMEM],
        compiler_params=PARAMS,
        name="blend",
    )(costs, raw)


def finish_kernel(plan, *refs):
    parts, out, wide = refs[:-2], refs[-2], refs[-1]
    n_rows = plan.spheres // 4
    for l in range(plan.here):
        at = plan.here * 3 * n_rows + l
        total = parts[0][at : at + 1, :]
        for p in parts[1:]:
            total = total + p[at : at + 1, :]
        inverse = 1.0 / total
        for c in range(3):
            at = (l * 3 + c) * n_rows
            y = parts[0][at : at + n_rows, :]
            for p in parts[1:]:
                y = y + p[at : at + n_rows, :]
            y = y * inverse
            for j in range(4):
                z = pltpu.roll(y, (LANES - j * W) % LANES, 1) if j else y
                wide[pl.ds(j, n_rows, stride=4), :] = z
            out[l, c] = wide[...].T[:W]


def finish(plan, parts):
    return pl.pallas_call(
        functools.partial(finish_kernel, plan),
        out_shape=jax.ShapeDtypeStruct((plan.here, 3, W, plan.spheres), jnp.float32),
        in_specs=[VMEM] * len(parts),
        out_specs=VMEM,
        scratch_shapes=[pltpu.VMEM((plan.spheres, LANES), jnp.float32)],
        compiler_params=PARAMS,
        name="finish",
    )(*parts)


def exchanged(block, axis, k):
    size = lax.axis_size(axis)
    return lax.ppermute(block, axis, [(i, i ^ k) for i in range(size)])


def local(centres, sphere_radius, counts, adjacency):
    here, _, spheres, columns = centres.shape
    plan = Plan(lax.axis_size("robot"), here, spheres, columns)
    stored = centres.reshape(here, 3, spheres, plan.tiles, LANES)
    stored = stored.transpose(1, 2, 3, 0, 4).reshape(-1, LANES)
    *chunks, raw = pack(plan, counts, sphere_radius, adjacency, stored)
    chunks = [chunks[0]] + [exchanged(chunks[k], "robot", k) for k in range(1, plan.group)]
    costs = cost(plan, chunks)
    costs = lax.all_to_all(costs, "robot", 0, 0, tiled=True)
    robot_cost, sums = blend(plan, costs, raw)
    parts = [sums] + [exchanged(sums, "seed", k) for k in range(1, lax.axis_size("seed"))]
    return robot_cost, finish(plan, parts).transpose(0, 1, 3, 2)


def solution(mesh):
    return jax.shard_map(
        local,
        mesh=mesh,
        in_specs=(P("robot", None, None, "seed"), P("robot", None), P("robot"), P("robot", None)),
        out_specs=(P("robot", "seed"), P("robot", None, None, None)),
        check_vma=False,
    )
```

```python
import functools
import math

import jax
import jax.numpy as jnp
from jax import lax
from jax.experimental import pallas as pl
from jax.experimental.pallas import tpu as pltpu
from jax.sharding import PartitionSpec as P

W = 32
LANES = 128
SUB = 8
SCALE = math.sqrt(math.log2(math.e))
FAR = 1e15
VMEM = pl.BlockSpec(memory_space=pltpu.VMEM)
SMEM = pl.BlockSpec(memory_space=pltpu.SMEM)
PARAMS = pltpu.CompilerParams(vmem_limit_bytes=16 * 1024 * 1024)


def round_up(value, step):
    return -(-value // step) * step


class Plan:
    def __init__(self, group, robots_here, spheres, columns):
        self.group = group
        self.chips = group // 2
        self.here = robots_here
        self.spheres = spheres
        self.columns = columns
        self.width = columns // group
        self.lane_groups = LANES // self.width
        self.rows = -(-spheres // self.lane_groups)
        self.padded = self.rows * self.lane_groups
        self.parts = -(-self.rows // SUB)
        self.slots = group * robots_here
        self.halves = -(-self.slots // 16)
        self.sweep_late = self.width % W == 0
        self.fields = 3 if self.sweep_late else 4
        self.data_rows = robots_here * self.fields * self.rows
        self.chunk_rows = round_up(self.data_rows + robots_here, SUB)
        self.tiles = columns // LANES


def iota(shape, axis):
    return lax.broadcasted_iota(jnp.int32, shape, axis)


def sweep(points, last, radius):
    squares = None
    middles = []
    for x in points:
        ahead = jnp.where(last, x, pltpu.roll(x, LANES - 1, 1))
        middles.append((0.5 * SCALE) * (x + ahead))
        square = (ahead - x) * (ahead - x)
        squares = square if squares is None else squares + square
    return middles, radius + 0.5 * jnp.sqrt(squares + 1e-06)


def pack_kernel(plan, counts, radius, adjacency, stored, mine, theirs, source):
    me = lax.axis_index("robot")
    n, g, rows, width = plan.spheres, plan.lane_groups, plan.rows, plan.width
    step = plan.tiles * plan.here
    order = iota((n, LANES), 0)
    for l in range(plan.here):
        for t in range(plan.tiles):
            points = [
                stored[pl.ds(c * n * step + t * plan.here + l, n, stride=step), :] for c in range(3)
            ]
            if not plan.sweep_late:
                diagonal = iota((n, n), 0) == iota((n, n), 1)
                column = jnp.sum(
                    jnp.where(diagonal, radius[l : l + 1, :], 0.0), axis=1, keepdims=True
                )
                points, swept = sweep(points, iota((n, LANES), 1) % W == W - 1, column)
                robot = me * plan.here + l
                off = FAR * (1 + order + plan.padded * robot).astype(jnp.float32)
                points[0] = jnp.where(order < counts[l], points[0], off)
                points.append(swept)
                spare = plan.padded - n
                if spare:
                    index = n + iota((spare, LANES), 0) + plan.padded * robot
                    fill = FAR * (1 + index).astype(jnp.float32)
                    for c in range(4):
                        source[t, l * 4 + c, n:, :] = fill if c == 0 else jnp.ones_like(fill)
            for c, x in enumerate(points):
                source[t, l * plan.fields + c, 0:n, :] = x
    lane = iota((1, LANES), 1)
    links = iota((1, plan.slots), 1)
    heads = []
    for l in range(plan.here):
        head = jnp.where(lane == n, counts[l].astype(jnp.float32), 0.0)
        for h in range(plan.halves):
            bits = jnp.where(
                (adjacency[l : l + 1, :] != 0) & (links // 16 == h), 1 << (links % 16), 0
            ).astype(jnp.float32)
            head = jnp.where(lane == n + 1 + h, jnp.sum(bits, axis=1, keepdims=True), head)
        heads.append(head)
    lane_group = iota((rows, LANES), 1) // width
    for k in range(plan.group):
        out = (mine, theirs)[k % 2]
        dest = me ^ k
        tile = dest // g
        spot = dest % g
        for f in range(plan.here * plan.fields):
            y = jnp.zeros((rows, LANES), jnp.float32)
            for j in range(g):
                x = source[tile, f, pl.ds(j, rows, stride=g), :]
                x = pltpu.roll(x, ((j + g - spot) % g) * width, 1)
                y = jnp.where(lane_group == j, x, y)
            out[k // 2, f * rows : (f + 1) * rows, :] = y
        for l in range(plan.here):
            at = plan.data_rows + l
            out[k // 2, at : at + 1, :] = heads[l]
            out[k // 2, at : at + 1, 0:n] = radius[l : l + 1, :]


def pack(plan, counts, radius, adjacency, stored):
    half = jax.ShapeDtypeStruct((plan.chips, plan.chunk_rows, LANES), jnp.float32)
    return pl.pallas_call(
        functools.partial(pack_kernel, plan),
        out_shape=[half, half],
        in_specs=[SMEM, VMEM, VMEM, VMEM],
        out_specs=[VMEM, VMEM],
        scratch_shapes=[
            pltpu.VMEM((plan.tiles, plan.here * plan.fields, plan.padded, LANES), jnp.float32)
        ],
        compiler_params=PARAMS,
        name="pack",
    )(counts, radius, adjacency, stored)


def join_kernel(plan, mine, theirs, *outs):
    for k in range(plan.chips):
        outs[k][0] = mine[k]
        outs[k][1] = theirs[k]


def join(plan, mine, theirs):
    pair = jax.ShapeDtypeStruct((2, plan.chunk_rows, LANES), jnp.float32)
    return pl.pallas_call(
        functools.partial(join_kernel, plan),
        out_shape=[pair] * plan.chips,
        in_specs=[VMEM, VMEM],
        out_specs=[VMEM] * plan.chips,
        compiler_params=PARAMS,
        name="join",
    )(mine, theirs)


def term(first, second):
    gap = first[0] - second[0]
    square = gap * gap
    for c in (1, 2):
        gap = first[c] - second[c]
        square = square + gap * gap
    inverse = 1.0 / (first[3] + second[3])
    return jnp.exp2(-(square * (inverse * inverse)))


def masked(value, keep):
    return value if keep is None else jnp.where(keep, value, 0.0)


def cost_kernel(plan, stage, *refs):
    chunks, refs = refs[: stage + 1], refs[stage + 1 :]
    known, refs = refs[:stage], refs[stage:]
    before, refs = refs[: 1 if stage else 0], refs[1 if stage else 0 :]
    ends = stage == plan.chips - 1
    if ends:
        out, blocks, packed, sums, totals, names, starts = refs
    else:
        blocks, totals, packed, sums, names, starts = refs
    me = lax.axis_index("robot")
    g, rows, width, here, n = plan.lane_groups, plan.rows, plan.width, plan.here, plan.spheres
    parts, fresh = plan.parts, 2 * plan.here
    first_slot = stage * fresh
    deep = parts * SUB

    def line_of(slot):
        at = plan.data_rows + slot % here
        return chunks[slot // fresh][slot % fresh // here, at : at + 1, :]

    for u in range(first_slot + fresh):
        count = line_of(u)[0, n].astype(jnp.int32)
        starts[u] = jnp.minimum((count + g - 1) // g, rows)
    for i in range(fresh):
        line = line_of(first_slot + i)
        links = [line[0, n + 1 + h].astype(jnp.int32) for h in range(plan.halves)]
        for k in range(stage + 1):
            found = jnp.int32(0)
            for v in range(fresh if k < stage else i):
                robot = (k * fresh + v) ^ (me * here)
                mask = links[0]
                for h in range(1, plan.halves):
                    mask = jnp.where(robot // 16 == h, links[h], mask)
                names[k, i, found] = v
                found = found + ((mask >> (robot % 16)) & 1)
            names[k, i, fresh] = found

    sphere = iota((rows, LANES), 0) * g + iota((rows, LANES), 1) // width
    last = iota((rows, LANES), 1) % W == W - 1
    for i in range(fresh):
        slot = first_slot + i
        chunk = chunks[stage].at[i // here]
        at = i % here * plan.fields * rows
        fields = [chunk[at + f * rows : at + (f + 1) * rows, :] for f in range(plan.fields)]
        if plan.sweep_late:
            line = line_of(slot)
            wide = jnp.broadcast_to(line, (SUB, LANES))
            pick = iota((SUB, LANES), 0) * g + iota((SUB, LANES), 1) // width
            radius = [
                jnp.take_along_axis(
                    wide, jnp.minimum(pick + p * SUB * g, LANES - 1), axis=1,
                    mode="promise_in_bounds",
                )
                for p in range(parts)
            ]
            fields, swept = sweep(fields, last, jnp.concatenate(radius, axis=0)[:rows])
            count = line[:, n : n + 1].astype(jnp.int32)
            off = FAR * (1 + sphere + plan.padded * slot).astype(jnp.float32)
            fields[0] = jnp.where(sphere < count, fields[0], off)
            fields.append(swept)
        for c in range(4):
            for m in range(g):
                x = fields[c]
                blocks[i, c, m, 0:rows, :] = pltpu.roll(x, m * width, 1) if m else x
            if deep > rows:
                fill = -FAR if c == 0 else 1.0
                blocks[i, c, 0, rows:deep, :] = jnp.full((deep - rows, LANES), fill, jnp.float32)
    for u in range(first_slot):
        totals[u] = before[0][u]
    for i in range(fresh):
        totals[first_slot + i] = jnp.zeros((SUB, LANES), jnp.float32)

    def row(i, m, r):
        return [blocks[i, c, m, r : r + 1, :] for c in range(4)]

    def part(i, m, p):
        return [blocks[i, c, m, p * SUB : (p + 1) * SUB, :] for c in range(4)]

    sub = iota((SUB, LANES), 0)
    lane_group = iota((SUB, LANES), 1) // width

    def self_terms(u, high):
        total = jnp.zeros((SUB, LANES), jnp.float32)
        second = part(u, 0, 0)
        turned = second
        for d in range(SUB // 2 + 1):
            if d:
                turned = [pltpu.roll(x, SUB - d, 0) for x in second]
            low = (sub + d) % SUB
            for m in range(g):
                other = (lane_group + g - m) % g
                if d == 0:
                    if m < 2:
                        continue
                    keep = lane_group >= m
                elif d == 1 and m == 1:
                    keep = jnp.abs((low - sub) * g + lane_group - other) >= 2
                elif 2 * d == SUB:
                    keep = sub < d
                else:
                    keep = None
                total = total + masked(term(part(u, m, 0), turned), keep)
        for r in range(SUB, high):
            for p in range(parts):
                if p * SUB > r:
                    continue
                second = part(u, 0, p)
                for m in range(g):
                    other = (lane_group + g - m) % g
                    ahead = (r - p * SUB - sub) * g + other - lane_group
                    near = r < (p + 1) * SUB + 1
                    total = total + masked(term(row(u, m, r), second), ahead >= 2 if near else None)
        return total

    def with_rows(u, trips, high):
        total = self_terms(u, high)

        def trip(j, total):
            at = pl.multiple_of(j * SUB, SUB)
            second = [packed[c, pl.ds(at, SUB), :] for c in range(4)]
            value = jnp.zeros((SUB, LANES), jnp.float32)
            for r in range(high):
                for m in range(g):
                    value = value + term(row(u, m, r), second)
            sums[pl.ds(at, SUB), :] = value
            return total + value

        totals[first_slot + u] = totals[first_slot + u] + lax.fori_loop(0, trips, trip, total)

    lowest = max(1, -(-(n // 2) // g))

    def choose(u, trips, low, high):
        if low == high:
            with_rows(u, trips, high)
            return
        middle = (low + high) // 2

        @pl.when(starts[first_slot + u] <= middle)
        def _():
            choose(u, trips, low, middle)

        @pl.when(starts[first_slot + u] > middle)
        def _():
            choose(u, trips, middle + 1, high)

    @pl.loop(0, fresh)
    def _(u):
        filled = jnp.int32(0)
        for k in range(stage + 1):

            def gather(e, filled, k=k):
                v = names[k, u, e]
                for c in range(4):
                    packed[c, pl.ds(filled, deep), :] = (known[k] if k < stage else blocks)[v, c, 0]
                return filled + starts[k * fresh + v]

            filled = lax.fori_loop(0, names[k, u, fresh], gather, filled)
        for c in range(4):
            fill = -FAR if c == 0 else 1.0
            packed[c, pl.ds(filled, SUB), :] = jnp.full((SUB, LANES), fill, jnp.float32)
        choose(u, (filled + SUB - 1) // SUB, lowest, rows)

        filled = jnp.int32(0)
        for k in range(stage + 1):

            def hand_out(e, filled, k=k):
                v = k * fresh + names[k, u, e]
                value = totals[v]
                for p in range(parts):
                    line = sums[pl.ds(filled + p * SUB, SUB), :]
                    value = value + jnp.where(sub + p * SUB < starts[v], line, 0.0)
                totals[v] = value
                return filled + starts[v]

            filled = lax.fori_loop(0, names[k, u, fresh], hand_out, filled)

    if not ends:
        return
    spot = iota((1, LANES), 1) // width == me % g
    for k in range(plan.group):
        for l in range(here):
            value = jnp.sum(totals[k * here + l], axis=0, keepdims=True)
            shift = width
            while shift < LANES:
                value = value + pltpu.roll(value, shift, 1)
                shift *= 2
            value = jnp.where(spot, value, 0.0) / (n * n)
            out[pl.ds((me ^ k) * here + l, 1), :] = value


def cost(plan, stage, chunks, known, before):
    fresh, g = 2 * plan.here, plan.lane_groups
    slots = (stage + 1) * fresh
    deep = plan.parts * SUB
    long = round_up(slots * plan.rows + deep + SUB, SUB)
    block = (fresh, 4, g, deep, LANES)
    total = (slots, SUB, LANES)
    ends = stage == plan.chips - 1
    if ends:
        out_shape = [jax.ShapeDtypeStruct((slots, LANES), jnp.float32)]
    else:
        out_shape = [jax.ShapeDtypeStruct(shape, jnp.float32) for shape in (block, total)]
    return pl.pallas_call(
        functools.partial(cost_kernel, plan, stage),
        out_shape=out_shape,
        in_specs=[VMEM] * (len(chunks) + len(known) + len(before)),
        out_specs=[VMEM] * len(out_shape),
        scratch_shapes=([pltpu.VMEM(block, jnp.float32)] if ends else [])
        + [pltpu.VMEM((4, long, LANES), jnp.float32), pltpu.VMEM((long, LANES), jnp.float32)]
        + ([pltpu.VMEM(total, jnp.float32)] if ends else [])
        + [
            pltpu.SMEM((stage + 1, fresh, fresh + 1), jnp.int32),
            pltpu.SMEM((slots,), jnp.int32),
        ],
        compiler_params=PARAMS,
        cost_estimate=pl.CostEstimate(
            flops=20_000_000 * (stage + 1), bytes_accessed=1000, transcendentals=0
        ),
        name=f"cost{stage}",
    )(*chunks, *known, *before)


def blend_kernel(plan, seeds_here, costs, stored, cost_out, sums):
    n, here, g = plan.spheres, plan.here, plan.lane_groups
    n_rows = n // 4
    step = plan.tiles * here
    seed_of = iota((seeds_here, LANES), 1) // W
    seed = iota((seeds_here, LANES), 0)
    fold = iota((n_rows, LANES), 1) // W
    per_tile = LANES // W
    for l in range(here):
        lines = []
        seed_cost = jnp.zeros((seeds_here, 1), jnp.float32)
        for t in range(plan.tiles):
            line = costs[t * g * here + l : t * g * here + l + 1, :]
            for d in range(t * g + 1, (t + 1) * g):
                line = line + costs[d * here + l : d * here + l + 1, :]
            cost_out[l : l + 1, t * LANES : (t + 1) * LANES] = line
            lines.append(line)
            mine = seed_of + t * per_tile == seed
            seed_cost = seed_cost + jnp.sum(jnp.where(mine, line, 0.0), axis=1, keepdims=True)
        weight = 1.0 / (1.0 + seed_cost)
        spread = []
        for t in range(plan.tiles):
            mine = seed_of + t * per_tile == seed
            spread.append(jnp.sum(jnp.where(mine, weight, 0.0), axis=0, keepdims=True))
        total = jnp.sum(weight, axis=0, keepdims=True)
        sums[here * 3 * n_rows + l : here * 3 * n_rows + l + 1, :] = jnp.broadcast_to(total, (1, LANES))
        for c in range(3):
            pieces = []
            for j in range(4):
                x = jnp.zeros((n_rows, LANES), jnp.float32)
                for t in range(plan.tiles):
                    at = (c * n + j) * step + t * here + l
                    x = x + stored[pl.ds(at, n_rows, stride=4 * step), :] * spread[t]
                pieces.append(x)
            y = jnp.zeros((n_rows, LANES), jnp.float32)
            for turn in range(4):
                z = pieces[0]
                for j in range(4):
                    z = jnp.where(fold == (j - turn) % 4, pieces[j], z)
                y = y + (pltpu.roll(z, turn * W, 1) if turn else z)
            at = (l * 3 + c) * n_rows
            sums[at : at + n_rows, :] = y


def blend(plan, costs, stored):
    seeds_here = plan.columns // W
    rows = round_up(plan.here * (3 * plan.spheres // 4 + 1), SUB)
    return pl.pallas_call(
        functools.partial(blend_kernel, plan, seeds_here),
        out_shape=[
            jax.ShapeDtypeStruct((plan.here, plan.columns), jnp.float32),
            jax.ShapeDtypeStruct((rows, LANES), jnp.float32),
        ],
        in_specs=[VMEM, VMEM],
        out_specs=[VMEM, VMEM],
        compiler_params=PARAMS,
        name="blend",
    )(costs, stored)


def finish_kernel(plan, *refs):
    parts, out, wide = refs[:-2], refs[-2], refs[-1]
    n_rows = plan.spheres // 4
    for l in range(plan.here):
        at = plan.here * 3 * n_rows + l
        total = parts[0][at : at + 1, :]
        for p in parts[1:]:
            total = total + p[at : at + 1, :]
        inverse = 1.0 / total
        for c in range(3):
            at = (l * 3 + c) * n_rows
            y = parts[0][at : at + n_rows, :]
            for p in parts[1:]:
                y = y + p[at : at + n_rows, :]
            y = y * inverse
            for j in range(4):
                z = pltpu.roll(y, (LANES - j * W) % LANES, 1) if j else y
                wide[l * 3 + c, pl.ds(j, n_rows, stride=4), :] = z
            out[l, c] = wide[l * 3 + c].T[:W]


def finish(plan, parts):
    return pl.pallas_call(
        functools.partial(finish_kernel, plan),
        out_shape=jax.ShapeDtypeStruct((plan.here, 3, W, plan.spheres), jnp.float32),
        in_specs=[VMEM] * len(parts),
        out_specs=VMEM,
        scratch_shapes=[pltpu.VMEM((plan.here * 3, plan.spheres, LANES), jnp.float32)],
        compiler_params=PARAMS,
        name="finish",
    )(*parts)


def exchanged(block, axis, k):
    size = lax.axis_size(axis)
    return lax.ppermute(block, axis, [(i, i ^ k) for i in range(size)])


def local(centres, sphere_radius, counts, adjacency):
    here, _, spheres, columns = centres.shape
    plan = Plan(lax.axis_size("robot"), here, spheres, columns)
    stored = centres.reshape(here, 3, spheres, plan.tiles, LANES)
    stored = stored.transpose(1, 2, 3, 0, 4).reshape(-1, LANES)
    mine, theirs = pack(plan, counts, sphere_radius, adjacency, stored)
    chunks = join(plan, mine, exchanged(theirs, "robot", 1))
    chunks = [chunks[0]] + [exchanged(chunks[k], "robot", 2 * k) for k in range(1, plan.chips)]
    known, before = [], []
    for stage in range(plan.chips - 1):
        block, total = cost(plan, stage, chunks[: stage + 1], known, before)
        known.append(block)
        before = [total]
    (costs,) = cost(plan, plan.chips - 1, chunks, known, before)
    costs = lax.all_to_all(costs, "robot", 0, 0, tiled=True)
    robot_cost, sums = blend(plan, costs, stored)
    parts = [sums] + [exchanged(sums, "seed", k) for k in range(1, lax.axis_size("seed"))]
    return robot_cost, finish(plan, parts).transpose(0, 1, 3, 2)


def solution(mesh):
    return jax.shard_map(
        local,
        mesh=mesh,
        in_specs=(P("robot", None, None, "seed"), P("robot", None), P("robot"), P("robot", None)),
        out_specs=(P("robot", "seed"), P("robot", None, None, None)),
        check_vma=False,
    )
```

```python
import functools
import math

import jax
import jax.numpy as jnp
from jax import lax
from jax.experimental import pallas as pl
from jax.experimental.pallas import tpu as pltpu
from jax.sharding import PartitionSpec as P

W = 32
LANES = 128
SUB = 8
SCALE = math.sqrt(math.log2(math.e))
FAR = 1e15
VMEM = pl.BlockSpec(memory_space=pltpu.VMEM)
SMEM = pl.BlockSpec(memory_space=pltpu.SMEM)
PARAMS = pltpu.CompilerParams(vmem_limit_bytes=16 * 1024 * 1024)


def round_up(value, step):
    return -(-value // step) * step


class Plan:
    def __init__(self, group, robots_here, spheres, columns):
        self.group = group
        self.chips = group // 2
        self.here = robots_here
        self.spheres = spheres
        self.columns = columns
        self.width = columns // group
        self.lane_groups = LANES // self.width
        self.rows = -(-spheres // self.lane_groups)
        self.padded = self.rows * self.lane_groups
        self.parts = -(-self.rows // SUB)
        self.slots = group * robots_here
        self.halves = -(-self.slots // 16)
        self.sweep_late = self.width % W == 0
        self.fields = 3 if self.sweep_late else 4
        self.data_rows = robots_here * self.fields * self.rows
        self.chunk_rows = round_up(self.data_rows + robots_here, SUB)
        self.tiles = columns // LANES


def iota(shape, axis):
    return lax.broadcasted_iota(jnp.int32, shape, axis)


def sweep(points, last, radius):
    squares = None
    middles = []
    for x in points:
        ahead = jnp.where(last, x, pltpu.roll(x, LANES - 1, 1))
        middles.append((0.5 * SCALE) * (x + ahead))
        square = (ahead - x) * (ahead - x)
        squares = square if squares is None else squares + square
    return middles, radius + 0.5 * jnp.sqrt(squares + 1e-06)


def pack_kernel(plan, counts_hbm, radius_hbm, adjacency_hbm, stored_hbm, mine, theirs, *scratch):
    counts, radius, adjacency, stored, source, sem = scratch
    me = lax.axis_index("robot")
    n, g, rows, width, here = plan.spheres, plan.lane_groups, plan.rows, plan.width, plan.here
    step = plan.tiles * here
    copies = [
        pltpu.make_async_copy(src, dst, sem.at[i])
        for i, (src, dst) in enumerate(
            zip((stored_hbm, counts_hbm, radius_hbm, adjacency_hbm), (stored, counts, radius, adjacency))
        )
    ]
    for copy in copies:
        copy.start()
    for copy in copies[1:]:
        copy.wait()
    lane = iota((1, LANES), 1)
    links = iota((1, plan.slots), 1)
    heads = []
    for l in range(here):
        head = jnp.where(lane == n, counts[:, l : l + 1].astype(jnp.float32), 0.0)
        for h in range(plan.halves):
            bits = jnp.where(
                (adjacency[l : l + 1, :] != 0) & (links // 16 == h), 1 << (links % 16), 0
            ).astype(jnp.float32)
            head = jnp.where(lane == n + 1 + h, jnp.sum(bits, axis=1, keepdims=True), head)
        heads.append(head)
    copies[0].wait()
    if not plan.sweep_late:
        order = iota((n, LANES), 0)
        diagonal = iota((n, n), 0) == iota((n, n), 1)
        for l in range(here):
            column = jnp.sum(jnp.where(diagonal, radius[l : l + 1, :], 0.0), axis=1, keepdims=True)
            robot = me * here + l
            off = FAR * (1 + order + plan.padded * robot).astype(jnp.float32)
            for t in range(plan.tiles):
                points = [
                    stored[pl.ds(c * n * step + t * here + l, n, stride=step), :] for c in range(3)
                ]
                fields, swept = sweep(points, iota((n, LANES), 1) % W == W - 1, column)
                fields[0] = jnp.where(order < counts[:, l : l + 1], fields[0], off)
                for c, x in enumerate(fields + [swept]):
                    source[t, l * 4 + c, 0:n, :] = x
                if plan.padded > n:
                    index = n + iota((plan.padded - n, LANES), 0) + plan.padded * robot
                    fill = FAR * (1 + index).astype(jnp.float32)
                    for c in range(4):
                        source[t, l * 4 + c, n:, :] = fill if c == 0 else jnp.ones_like(fill)
    lane_group = iota((rows, LANES), 1) // width
    for k in [*range(1, plan.group, 2), *range(0, plan.group, 2)]:
        out = (mine, theirs)[k % 2]
        dest = me ^ k
        tile = dest // g
        spot = dest % g
        for l in range(here):
            for c in range(plan.fields):
                y = jnp.zeros((rows, LANES), jnp.float32)
                for j in range(g):
                    if plan.sweep_late:
                        at = (c * n + j) * step + tile * here + l
                        x = stored[pl.ds(at, rows, stride=g * step), :]
                    else:
                        x = source[tile, l * 4 + c, pl.ds(j, rows, stride=g), :]
                    x = pltpu.roll(x, ((j + g - spot) % g) * width, 1)
                    y = jnp.where(lane_group == j, x, y)
                at = (l * plan.fields + c) * rows
                out[k // 2, at : at + rows, :] = y
            at = plan.data_rows + l
            out[k // 2, at : at + 1, :] = heads[l]
            out[k // 2, at : at + 1, 0:n] = radius[l : l + 1, :]


def pack(plan, counts, radius, adjacency, stored):
    half = jax.ShapeDtypeStruct((plan.chips, plan.chunk_rows, LANES), jnp.float32)
    args = (counts.reshape(1, -1), radius, adjacency, stored)
    swept = (plan.tiles, plan.here * 4, plan.padded, LANES)
    return pl.pallas_call(
        functools.partial(pack_kernel, plan),
        out_shape=[half, half],
        in_specs=[pl.BlockSpec(memory_space=pltpu.HBM)] * len(args),
        out_specs=[VMEM, VMEM],
        scratch_shapes=[pltpu.VMEM(x.shape, x.dtype) for x in args]
        + [
            pltpu.VMEM((SUB, LANES) if plan.sweep_late else swept, jnp.float32),
            pltpu.SemaphoreType.DMA((len(args),)),
        ],
        compiler_params=PARAMS,
        name="pack",
    )(*args)


def join_kernel(plan, mine, theirs, *outs):
    for k in range(plan.chips):
        outs[k][0] = mine[k]
        outs[k][1] = theirs[k]


def join(plan, mine, theirs):
    pair = jax.ShapeDtypeStruct((2, plan.chunk_rows, LANES), jnp.float32)
    return pl.pallas_call(
        functools.partial(join_kernel, plan),
        out_shape=[pair] * plan.chips,
        in_specs=[VMEM, VMEM],
        out_specs=[VMEM] * plan.chips,
        compiler_params=PARAMS,
        name="join",
    )(mine, theirs)


def term(first, second):
    gap = first[0] - second[0]
    square = gap * gap
    for c in (1, 2):
        gap = first[c] - second[c]
        square = square + gap * gap
    inverse = 1.0 / (first[3] + second[3])
    return jnp.exp2(-(square * (inverse * inverse)))


def masked(value, keep):
    return value if keep is None else jnp.where(keep, value, 0.0)


def cost_kernel(plan, stage, *refs):
    chunks, refs = refs[: stage + 1], refs[stage + 1 :]
    before, refs = refs[: 2 if stage else 0], refs[2 if stage else 0 :]
    ends = stage == plan.chips - 1
    if ends:
        out, store, totals, blocks, tails, sums, starts, links = refs
    else:
        store, totals, blocks, tails, sums, starts, links = refs
    me = lax.axis_index("robot")
    g, rows, width, here, n = plan.lane_groups, plan.rows, plan.width, plan.here, plan.spheres
    parts, fresh = plan.parts, 2 * plan.here
    first_slot = stage * fresh
    deep = parts * SUB

    def line_of(slot):
        at = plan.data_rows + slot % here
        return chunks[slot // fresh][slot % fresh // here, at : at + 1, :]

    for u in range(first_slot + fresh):
        count = line_of(u)[0, n].astype(jnp.int32)
        starts[u] = jnp.minimum((count + g - 1) // g, rows)
    for i in range(fresh):
        line = line_of(first_slot + i)
        bits = line[0, n + 1].astype(jnp.int32)
        for h in range(1, plan.halves):
            bits = bits | (line[0, n + 1 + h].astype(jnp.int32) << (16 * h))
        step = 1
        while step < plan.slots:
            low = sum(1 << b for b in range(plan.slots) if not b & step)
            low = low - (1 << 32) if low >= 1 << 31 else low
            turned = ((bits & low) << step) | ((bits >> step) & low)
            bits = jnp.where((me * here) & step != 0, turned, bits)
            step *= 2
        links[i] = bits & ((1 << (first_slot + i)) - 1)

    sphere = iota((rows, LANES), 0) * g + iota((rows, LANES), 1) // width
    last = iota((rows, LANES), 1) % W == W - 1
    for i in range(fresh):
        slot = first_slot + i
        chunk = chunks[stage].at[i // here]
        at = i % here * plan.fields * rows
        fields = [chunk[at + f * rows : at + (f + 1) * rows, :] for f in range(plan.fields)]
        if plan.sweep_late:
            line = line_of(slot)
            wide = jnp.broadcast_to(line, (SUB, LANES))
            pick = iota((SUB, LANES), 0) * g + iota((SUB, LANES), 1) // width
            radius = [
                jnp.take_along_axis(
                    wide, jnp.minimum(pick + p * SUB * g, LANES - 1), axis=1,
                    mode="promise_in_bounds",
                )
                for p in range(parts)
            ]
            fields, swept = sweep(fields, last, jnp.concatenate(radius, axis=0)[:rows])
            count = line[:, n : n + 1].astype(jnp.int32)
            off = FAR * (1 + sphere + plan.padded * slot).astype(jnp.float32)
            fields[0] = jnp.where(sphere < count, fields[0], off)
            fields.append(swept)
        for c in range(4):
            x = fields[c]
            for m in range(g):
                blocks[i, c, m, 0:rows, :] = pltpu.roll(x, m * width, 1) if m else x
            store[slot, c, 0:rows, :] = x
            if deep > rows:
                fill = jnp.full((deep - rows, LANES), -FAR if c == 0 else 1.0, jnp.float32)
                store[slot, c, rows:deep, :] = fill
        totals[slot] = jnp.zeros((SUB, LANES), jnp.float32)
    for u in range(first_slot):
        store[u] = before[0][u]
        totals[u] = before[1][u]

    def row(i, m, r):
        return [blocks[i, c, m, r : r + 1, :] for c in range(4)]

    def part(slot, p):
        return [store[slot, c, p * SUB : (p + 1) * SUB, :] for c in range(4)]

    sub = iota((SUB, LANES), 0)
    lane_group = iota((SUB, LANES), 1) // width
    nothing = jnp.zeros((SUB, LANES), jnp.float32)

    def self_terms(u, high):
        total = nothing
        second = part(first_slot + u, 0)
        for d in range(SUB // 2 + 1):
            turned = [pltpu.roll(x, SUB - d, 0) for x in second] if d else second
            low = (sub + d) % SUB
            for m in range(g):
                other = (lane_group + g - m) % g
                if d == 0:
                    if m < 2:
                        continue
                    keep = lane_group >= m
                elif d == 1 and m == 1:
                    keep = jnp.abs((low - sub) * g + lane_group - other) >= 2
                elif 2 * d == SUB:
                    keep = sub < d
                else:
                    keep = None
                first = [blocks[u, c, m, 0:SUB, :] for c in range(4)]
                total = total + masked(term(first, turned), keep)
        for r in range(SUB, high):
            for p in range(parts):
                if p * SUB > r:
                    continue
                second = part(first_slot + u, p)
                for m in range(g):
                    other = (lane_group + g - m) % g
                    ahead = (r - p * SUB - sub) * g + other - lane_group
                    near = r < (p + 1) * SUB + 1
                    total = total + masked(term(row(u, m, r), second), ahead >= 2 if near else None)
        return total

    def against(u, high, second):
        value = nothing
        for r in range(high):
            for m in range(g):
                value = value + term(row(u, m, r), second)
        return value

    def lowest_bit(bits):
        return 31 - lax.clz(bits & -bits)

    def with_rows(u, high):
        total = self_terms(u, high)

        def neighbour(state):
            bits, filled, total = state
            v = lowest_bit(bits)
            value = against(u, high, part(v, 0))
            totals[v] = totals[v] + value
            if parts > 1:
                for c, x in enumerate(part(v, 1)):
                    tails[c, pl.ds(filled, SUB), :] = x
                filled = filled + jnp.maximum(starts[v] - SUB, 0)
            return bits & (bits - 1), filled, total + value

        state = (links[u], jnp.int32(0), total)
        _, filled, total = lax.while_loop(lambda state: state[0] != 0, neighbour, state)
        if parts > 1:
            for c in range(4):
                fill = jnp.full((SUB, LANES), -FAR if c == 0 else 1.0, jnp.float32)
                tails[c, pl.ds(filled, SUB), :] = fill

            def trip(j, total):
                at = pl.multiple_of(j * SUB, SUB)
                value = against(u, high, [tails[c, pl.ds(at, SUB), :] for c in range(4)])
                sums[pl.ds(at, SUB), :] = value
                return total + value

            total = lax.fori_loop(0, (filled + SUB - 1) // SUB, trip, total)
        totals[first_slot + u] = totals[first_slot + u] + total

    lowest = max(1, -(-(n // 2) // g))

    def choose(u, low, high):
        if low == high:
            with_rows(u, high)
            return
        middle = (low + high) // 2

        @pl.when(starts[first_slot + u] <= middle)
        def _():
            choose(u, low, middle)

        @pl.when(starts[first_slot + u] > middle)
        def _():
            choose(u, middle + 1, high)

    @pl.loop(0, fresh)
    def _(u):
        choose(u, lowest, rows)
        if parts > 1:

            def hand_out(state):
                bits, filled = state
                v = lowest_bit(bits)
                more = jnp.maximum(starts[v] - SUB, 0)
                totals[v] = totals[v] + jnp.where(sub < more, sums[pl.ds(filled, SUB), :], 0.0)
                return bits & (bits - 1), filled + more

            lax.while_loop(lambda state: state[0] != 0, hand_out, (links[u], jnp.int32(0)))

    if not ends:
        return
    spot = iota((1, LANES), 1) // width == me % g
    for k in range(plan.group):
        for l in range(here):
            value = jnp.sum(totals[k * here + l], axis=0, keepdims=True)
            shift = width
            while shift < LANES:
                value = value + pltpu.roll(value, shift, 1)
                shift *= 2
            value = jnp.where(spot, value, 0.0) / (n * n)
            out[pl.ds((me ^ k) * here + l, 1), :] = value


def cost(plan, stage, chunks, before):
    fresh, g = 2 * plan.here, plan.lane_groups
    slots = (stage + 1) * fresh
    deep = plan.parts * SUB
    long = round_up(slots * max(plan.rows - SUB, 0) + 2 * SUB, SUB)
    carried = [(slots, 4, deep, LANES), (slots, SUB, LANES)]
    ends = stage == plan.chips - 1
    outs = [(slots, LANES)] if ends else carried
    scratch = (carried if ends else []) + [(fresh, 4, g, deep, LANES), (4, long, LANES), (long, LANES)]
    return pl.pallas_call(
        functools.partial(cost_kernel, plan, stage),
        out_shape=[jax.ShapeDtypeStruct(shape, jnp.float32) for shape in outs],
        in_specs=[VMEM] * (len(chunks) + len(before)),
        out_specs=[VMEM] * len(outs),
        scratch_shapes=[pltpu.VMEM(shape, jnp.float32) for shape in scratch]
        + [pltpu.SMEM((slots,), jnp.int32), pltpu.SMEM((fresh,), jnp.int32)],
        compiler_params=PARAMS,
        cost_estimate=pl.CostEstimate(
            flops=20_000_000 * (stage + 1), bytes_accessed=1000, transcendentals=0
        ),
        name=f"cost{stage}",
    )(*chunks, *before)


def blend_kernel(plan, seeds_here, costs, stored, cost_out, sums):
    n, here, g = plan.spheres, plan.here, plan.lane_groups
    n_rows = n // 4
    step = plan.tiles * here
    seed_of = iota((seeds_here, LANES), 1) // W
    seed = iota((seeds_here, LANES), 0)
    fold = iota((n_rows, LANES), 1) // W
    per_tile = LANES // W
    for l in range(here):
        lines = []
        seed_cost = jnp.zeros((seeds_here, 1), jnp.float32)
        for t in range(plan.tiles):
            line = costs[t * g * here + l : t * g * here + l + 1, :]
            for d in range(t * g + 1, (t + 1) * g):
                line = line + costs[d * here + l : d * here + l + 1, :]
            cost_out[l : l + 1, t * LANES : (t + 1) * LANES] = line
            lines.append(line)
            mine = seed_of + t * per_tile == seed
            seed_cost = seed_cost + jnp.sum(jnp.where(mine, line, 0.0), axis=1, keepdims=True)
        weight = 1.0 / (1.0 + seed_cost)
        spread = []
        for t in range(plan.tiles):
            mine = seed_of + t * per_tile == seed
            spread.append(jnp.sum(jnp.where(mine, weight, 0.0), axis=0, keepdims=True))
        total = jnp.sum(weight, axis=0, keepdims=True)
        sums[here * 3 * n_rows + l : here * 3 * n_rows + l + 1, :] = jnp.broadcast_to(total, (1, LANES))
        for c in range(3):
            pieces = []
            for j in range(4):
                x = jnp.zeros((n_rows, LANES), jnp.float32)
                for t in range(plan.tiles):
                    at = (c * n + j) * step + t * here + l
                    x = x + stored[pl.ds(at, n_rows, stride=4 * step), :] * spread[t]
                pieces.append(x)
            y = jnp.zeros((n_rows, LANES), jnp.float32)
            for turn in range(4):
                z = pieces[0]
                for j in range(4):
                    z = jnp.where(fold == (j - turn) % 4, pieces[j], z)
                y = y + (pltpu.roll(z, turn * W, 1) if turn else z)
            at = (l * 3 + c) * n_rows
            sums[at : at + n_rows, :] = y


def blend(plan, costs, stored):
    seeds_here = plan.columns // W
    rows = round_up(plan.here * (3 * plan.spheres // 4 + 1), SUB)
    return pl.pallas_call(
        functools.partial(blend_kernel, plan, seeds_here),
        out_shape=[
            jax.ShapeDtypeStruct((plan.here, plan.columns), jnp.float32),
            jax.ShapeDtypeStruct((rows, LANES), jnp.float32),
        ],
        in_specs=[VMEM, VMEM],
        out_specs=[VMEM, VMEM],
        compiler_params=PARAMS,
        name="blend",
    )(costs, stored)


def finish_kernel(plan, *refs):
    parts, out, wide = refs[:-2], refs[-2], refs[-1]
    n_rows = plan.spheres // 4
    for l in range(plan.here):
        at = plan.here * 3 * n_rows + l
        total = parts[0][at : at + 1, :]
        for p in parts[1:]:
            total = total + p[at : at + 1, :]
        inverse = 1.0 / total
        for c in range(3):
            at = (l * 3 + c) * n_rows
            y = parts[0][at : at + n_rows, :]
            for p in parts[1:]:
                y = y + p[at : at + n_rows, :]
            y = y * inverse
            for j in range(4):
                z = pltpu.roll(y, (LANES - j * W) % LANES, 1) if j else y
                wide[l * 3 + c, pl.ds(j, n_rows, stride=4), :] = z
            out[l, c] = wide[l * 3 + c].T[:W]


def finish(plan, parts):
    return pl.pallas_call(
        functools.partial(finish_kernel, plan),
        out_shape=jax.ShapeDtypeStruct((plan.here, 3, W, plan.spheres), jnp.float32),
        in_specs=[VMEM] * len(parts),
        out_specs=VMEM,
        scratch_shapes=[pltpu.VMEM((plan.here * 3, plan.spheres, LANES), jnp.float32)],
        compiler_params=PARAMS,
        name="finish",
    )(*parts)


def exchanged(block, axis, k):
    size = lax.axis_size(axis)
    return lax.ppermute(block, axis, [(i, i ^ k) for i in range(size)])


def local(centres, sphere_radius, counts, adjacency):
    here, _, spheres, columns = centres.shape
    plan = Plan(lax.axis_size("robot"), here, spheres, columns)
    stored = centres.reshape(here, 3, spheres, plan.tiles, LANES)
    stored = stored.transpose(1, 2, 3, 0, 4).reshape(-1, LANES)
    mine, theirs = pack(plan, counts, sphere_radius, adjacency, stored)
    chunks = join(plan, mine, exchanged(theirs, "robot", 1))
    chunks = [chunks[0]] + [exchanged(chunks[k], "robot", 2 * k) for k in range(1, plan.chips)]
    carried = []
    for stage in range(plan.chips):
        carried = cost(plan, stage, chunks[: stage + 1], carried)
    (costs,) = carried
    costs = lax.all_to_all(costs, "robot", 0, 0, tiled=True)
    robot_cost, sums = blend(plan, costs, stored)
    parts = [sums] + [exchanged(sums, "seed", k) for k in range(1, lax.axis_size("seed"))]
    return robot_cost, finish(plan, parts).transpose(0, 1, 3, 2)


def solution(mesh):
    return jax.shard_map(
        local,
        mesh=mesh,
        in_specs=(P("robot", None, None, "seed"), P("robot", None), P("robot"), P("robot", None)),
        out_specs=(P("robot", "seed"), P("robot", None, None, None)),
        check_vma=False,
    )
```

```python
import functools
import math

import jax
import jax.numpy as jnp
from jax import lax
from jax.experimental import pallas as pl
from jax.experimental.pallas import tpu as pltpu
from jax.sharding import PartitionSpec as P

W = 32
LANES = 128
SUB = 8
SCALE = math.sqrt(math.log2(math.e))
FAR = 1e15
VMEM = pl.BlockSpec(memory_space=pltpu.VMEM)
SMEM = pl.BlockSpec(memory_space=pltpu.SMEM)
PARAMS = pltpu.CompilerParams(vmem_limit_bytes=16 * 1024 * 1024)


def round_up(value, step):
    return -(-value // step) * step


class Plan:
    def __init__(self, group, robots_here, spheres, columns):
        self.group = group
        self.chips = group // 2
        self.here = robots_here
        self.spheres = spheres
        self.columns = columns
        self.width = columns // group
        self.lane_groups = LANES // self.width
        self.rows = -(-spheres // self.lane_groups)
        self.padded = self.rows * self.lane_groups
        self.parts = -(-self.rows // SUB)
        self.slots = group * robots_here
        self.halves = -(-self.slots // 16)
        self.sweep_late = self.width % W == 0
        self.fields = 3 if self.sweep_late else 4
        self.data_rows = robots_here * self.fields * self.rows
        self.chunk_rows = round_up(self.data_rows + robots_here, SUB)
        self.tiles = columns // LANES

    def arrival(self, stage):
        k = stage if stage < 2 else 2 * (stage - 1)
        return k * self.here, self.here if stage < 2 else 2 * self.here


def iota(shape, axis):
    return lax.broadcasted_iota(jnp.int32, shape, axis)


def sweep(points, last, radius):
    squares = None
    middles = []
    for x in points:
        ahead = jnp.where(last, x, pltpu.roll(x, LANES - 1, 1))
        middles.append((0.5 * SCALE) * (x + ahead))
        square = (ahead - x) * (ahead - x)
        squares = square if squares is None else squares + square
    return middles, radius + 0.5 * jnp.sqrt(squares + 1e-06)


def fetch(plan, sources, stored, lines, counts, radius, adjacency, sem):
    n = plan.spheres
    copies = [
        pltpu.make_async_copy(src, dst, sem.at[i])
        for i, (src, dst) in enumerate(zip(sources, (stored, counts, radius, adjacency)))
    ]
    for copy in copies:
        copy.start()
    for copy in copies[1:]:
        copy.wait()
    lane = iota((1, LANES), 1)
    links = iota((1, plan.slots), 1)
    for l in range(plan.here):
        head = jnp.where(lane == n, counts[:, l : l + 1].astype(jnp.float32), 0.0)
        for h in range(plan.halves):
            bits = jnp.where(
                (adjacency[l : l + 1, :] != 0) & (links // 16 == h), 1 << (links % 16), 0
            ).astype(jnp.float32)
            head = jnp.where(lane == n + 1 + h, jnp.sum(bits, axis=1, keepdims=True), head)
        lines[l : l + 1, :] = head
        lines[l : l + 1, 0:n] = radius[l : l + 1, :]
    copies[0].wait()


def pack_kernel(plan, core, *refs):
    if core:
        out, stored, lines, source = refs[4:8]
        fetch(plan, refs[:4], stored, lines, *refs[8:])
    else:
        lines, stored, out, source = refs
    me = lax.axis_index("robot")
    n, g, rows, width, here = plan.spheres, plan.lane_groups, plan.rows, plan.width, plan.here
    step = plan.tiles * here
    if not plan.sweep_late:
        order = iota((n, LANES), 0)
        diagonal = iota((n, n), 0) == iota((n, n), 1)
        for l in range(here):
            column = jnp.sum(jnp.where(diagonal, lines[l : l + 1, 0:n], 0.0), axis=1, keepdims=True)
            count = lines[l : l + 1, n : n + 1].astype(jnp.int32)
            robot = me * here + l
            off = FAR * (1 + order + plan.padded * robot).astype(jnp.float32)
            for t in range(plan.tiles):
                points = [
                    stored[pl.ds(c * n * step + t * here + l, n, stride=step), :] for c in range(3)
                ]
                fields, swept = sweep(points, iota((n, LANES), 1) % W == W - 1, column)
                fields[0] = jnp.where(order < count, fields[0], off)
                for c, x in enumerate(fields + [swept]):
                    source[t, l * 4 + c, 0:n, :] = x
                if plan.padded > n:
                    index = n + iota((plan.padded - n, LANES), 0) + plan.padded * robot
                    fill = FAR * (1 + index).astype(jnp.float32)
                    for c in range(4):
                        source[t, l * 4 + c, n:, :] = fill if c == 0 else jnp.ones_like(fill)
    lane_group = iota((rows, LANES), 1) // width
    for k in range(plan.chips):
        dest = me ^ (2 * k + core)
        tile = dest // g
        spot = dest % g
        for l in range(here):
            for c in range(plan.fields):
                y = jnp.zeros((rows, LANES), jnp.float32)
                for j in range(g):
                    if plan.sweep_late:
                        at = (c * n + j) * step + tile * here + l
                        x = stored[pl.ds(at, rows, stride=g * step), :]
                    else:
                        x = source[tile, l * 4 + c, pl.ds(j, rows, stride=g), :]
                    x = pltpu.roll(x, ((j + g - spot) % g) * width, 1)
                    y = jnp.where(lane_group == j, x, y)
                at = (l * plan.fields + c) * rows
                out[k, at : at + rows, :] = y
            at = plan.data_rows + l
            out[k, at : at + 1, :] = lines[l : l + 1, :]


def pack(plan, core, *args):
    shapes = [(plan.chips, plan.chunk_rows, LANES)]
    swept = (plan.tiles, plan.here * 4, plan.padded, LANES)
    scratch = [pltpu.VMEM((SUB, LANES) if plan.sweep_late else swept, jnp.float32)]
    specs = [VMEM, VMEM]
    if core:
        shapes += [args[0].shape, (plan.here, LANES)]
        scratch += [pltpu.VMEM(x.shape, x.dtype) for x in args[1:]]
        scratch += [pltpu.SemaphoreType.DMA((len(args),))]
        specs = [pl.BlockSpec(memory_space=pltpu.HBM)] * len(args)
        args = [pltpu.with_memory_space_constraint(x, pltpu.HBM) for x in args]
    return pl.pallas_call(
        functools.partial(pack_kernel, plan, core),
        out_shape=[jax.ShapeDtypeStruct(shape, jnp.float32) for shape in shapes],
        in_specs=specs,
        out_specs=[VMEM] * len(shapes),
        scratch_shapes=scratch,
        compiler_params=PARAMS,
        cost_estimate=pl.CostEstimate(flops=4_000_000, bytes_accessed=1000, transcendentals=0),
        name=f"pack{core}",
    )(*args)


def join_kernel(plan, mine, theirs, *outs):
    for k in range(1, plan.chips):
        outs[k - 1][0] = mine[k]
        outs[k - 1][1] = theirs[k]


def join(plan, mine, theirs):
    pair = jax.ShapeDtypeStruct((2, plan.chunk_rows, LANES), jnp.float32)
    return pl.pallas_call(
        functools.partial(join_kernel, plan),
        out_shape=[pair] * (plan.chips - 1),
        in_specs=[VMEM, VMEM],
        out_specs=[VMEM] * (plan.chips - 1),
        compiler_params=PARAMS,
        name="join",
    )(mine, theirs)


def term(first, second):
    gap = first[0] - second[0]
    square = gap * gap
    for c in (1, 2):
        gap = first[c] - second[c]
        square = square + gap * gap
    inverse = 1.0 / (first[3] + second[3])
    return jnp.exp2(-(square * (inverse * inverse)))


def masked(value, keep):
    return value if keep is None else jnp.where(keep, value, 0.0)


def cost_kernel(plan, stage, *refs):
    chunks, refs = refs[: stage + 1], refs[stage + 1 :]
    before, refs = refs[: 2 if stage else 0], refs[2 if stage else 0 :]
    ends = stage == plan.chips
    if ends:
        out, store, totals, blocks, tails, sums, starts, links = refs
    else:
        store, totals, blocks, tails, sums, starts, links = refs
    me = lax.axis_index("robot")
    g, rows, width, here, n = plan.lane_groups, plan.rows, plan.width, plan.here, plan.spheres
    parts = plan.parts
    first_slot, fresh = plan.arrival(stage)
    deep = parts * SUB

    def chunk_of(slot):
        k = slot // here
        return chunks[k].at[0] if k < 2 else chunks[k // 2 + 1].at[k % 2]

    def line_of(slot):
        at = plan.data_rows + slot % here
        return chunk_of(slot)[at : at + 1, :]

    for u in range(first_slot + fresh):
        count = line_of(u)[0, n].astype(jnp.int32)
        starts[u] = jnp.minimum((count + g - 1) // g, rows)
    for i in range(fresh):
        line = line_of(first_slot + i)
        bits = line[0, n + 1].astype(jnp.int32)
        for h in range(1, plan.halves):
            bits = bits | (line[0, n + 1 + h].astype(jnp.int32) << (16 * h))
        step = 1
        while step < plan.slots:
            low = sum(1 << b for b in range(plan.slots) if not b & step)
            low = low - (1 << 32) if low >= 1 << 31 else low
            turned = ((bits & low) << step) | ((bits >> step) & low)
            bits = jnp.where((me * here) & step != 0, turned, bits)
            step *= 2
        links[i] = bits & ((1 << (first_slot + i)) - 1)

    sphere = iota((rows, LANES), 0) * g + iota((rows, LANES), 1) // width
    last = iota((rows, LANES), 1) % W == W - 1
    for i in range(fresh):
        slot = first_slot + i
        chunk = chunk_of(slot)
        at = slot % here * plan.fields * rows
        fields = [chunk[at + f * rows : at + (f + 1) * rows, :] for f in range(plan.fields)]
        if plan.sweep_late:
            line = line_of(slot)
            wide = jnp.broadcast_to(line, (SUB, LANES))
            pick = iota((SUB, LANES), 0) * g + iota((SUB, LANES), 1) // width
            radius = [
                jnp.take_along_axis(
                    wide, jnp.minimum(pick + p * SUB * g, LANES - 1), axis=1,
                    mode="promise_in_bounds",
                )
                for p in range(parts)
            ]
            fields, swept = sweep(fields, last, jnp.concatenate(radius, axis=0)[:rows])
            count = line[:, n : n + 1].astype(jnp.int32)
            off = FAR * (1 + sphere + plan.padded * slot).astype(jnp.float32)
            fields[0] = jnp.where(sphere < count, fields[0], off)
            fields.append(swept)
        for c in range(4):
            x = fields[c]
            for m in range(g):
                blocks[i, c, m, 0:rows, :] = pltpu.roll(x, m * width, 1) if m else x
            store[slot, c, 0:rows, :] = x
            if deep > rows:
                fill = jnp.full((deep - rows, LANES), -FAR if c == 0 else 1.0, jnp.float32)
                store[slot, c, rows:deep, :] = fill
        totals[slot] = jnp.zeros((SUB, LANES), jnp.float32)
    for u in range(first_slot):
        store[u] = before[0][u]
        totals[u] = before[1][u]

    def row(i, m, r):
        return [blocks[i, c, m, r : r + 1, :] for c in range(4)]

    def part(slot, p):
        return [store[slot, c, p * SUB : (p + 1) * SUB, :] for c in range(4)]

    sub = iota((SUB, LANES), 0)
    lane_group = iota((SUB, LANES), 1) // width
    nothing = jnp.zeros((SUB, LANES), jnp.float32)

    def self_terms(u, high):
        total = nothing
        second = part(first_slot + u, 0)
        for d in range(SUB // 2 + 1):
            turned = [pltpu.roll(x, SUB - d, 0) for x in second] if d else second
            low = (sub + d) % SUB
            for m in range(g):
                other = (lane_group + g - m) % g
                if d == 0:
                    if m < 2:
                        continue
                    keep = lane_group >= m
                elif d == 1 and m == 1:
                    keep = jnp.abs((low - sub) * g + lane_group - other) >= 2
                elif 2 * d == SUB:
                    keep = sub < d
                else:
                    keep = None
                first = [blocks[u, c, m, 0:SUB, :] for c in range(4)]
                total = total + masked(term(first, turned), keep)
        for r in range(SUB, high):
            for p in range(parts):
                if p * SUB > r:
                    continue
                second = part(first_slot + u, p)
                for m in range(g):
                    other = (lane_group + g - m) % g
                    ahead = (r - p * SUB - sub) * g + other - lane_group
                    near = r < (p + 1) * SUB + 1
                    total = total + masked(term(row(u, m, r), second), ahead >= 2 if near else None)
        return total

    def against(u, high, second):
        value = nothing
        for r in range(high):
            for m in range(g):
                value = value + term(row(u, m, r), second)
        return value

    def lowest_bit(bits):
        return 31 - lax.clz(bits & -bits)

    def with_rows(u, high):
        total = self_terms(u, high)

        def neighbour(state):
            bits, filled, total = state
            v = lowest_bit(bits)
            value = against(u, high, part(v, 0))
            totals[v] = totals[v] + value
            if parts > 1:
                for c, x in enumerate(part(v, 1)):
                    tails[c, pl.ds(filled, SUB), :] = x
                filled = filled + jnp.maximum(starts[v] - SUB, 0)
            return bits & (bits - 1), filled, total + value

        state = (links[u], jnp.int32(0), total)
        _, filled, total = lax.while_loop(lambda state: state[0] != 0, neighbour, state)
        if parts > 1:
            for c in range(4):
                fill = jnp.full((SUB, LANES), -FAR if c == 0 else 1.0, jnp.float32)
                tails[c, pl.ds(filled, SUB), :] = fill

            def trip(j, total):
                at = pl.multiple_of(j * SUB, SUB)
                value = against(u, high, [tails[c, pl.ds(at, SUB), :] for c in range(4)])
                sums[pl.ds(at, SUB), :] = value
                return total + value

            total = lax.fori_loop(0, (filled + SUB - 1) // SUB, trip, total)
        totals[first_slot + u] = totals[first_slot + u] + total

    lowest = max(1, -(-(n // 2) // g))

    def choose(u, low, high):
        if low == high:
            with_rows(u, high)
            return
        middle = (low + high) // 2

        @pl.when(starts[first_slot + u] <= middle)
        def _():
            choose(u, low, middle)

        @pl.when(starts[first_slot + u] > middle)
        def _():
            choose(u, middle + 1, high)

    @pl.loop(0, fresh)
    def _(u):
        choose(u, lowest, rows)
        if parts > 1:

            def hand_out(state):
                bits, filled = state
                v = lowest_bit(bits)
                more = jnp.maximum(starts[v] - SUB, 0)
                totals[v] = totals[v] + jnp.where(sub < more, sums[pl.ds(filled, SUB), :], 0.0)
                return bits & (bits - 1), filled + more

            lax.while_loop(lambda state: state[0] != 0, hand_out, (links[u], jnp.int32(0)))

    if not ends:
        return
    spot = iota((1, LANES), 1) // width == me % g
    for k in range(plan.group):
        for l in range(here):
            value = jnp.sum(totals[k * here + l], axis=0, keepdims=True)
            shift = width
            while shift < LANES:
                value = value + pltpu.roll(value, shift, 1)
                shift *= 2
            value = jnp.where(spot, value, 0.0) / (n * n)
            out[pl.ds((me ^ k) * here + l, 1), :] = value


def cost(plan, stage, chunks, before):
    first_slot, fresh = plan.arrival(stage)
    slots, g = first_slot + fresh, plan.lane_groups
    deep = plan.parts * SUB
    long = round_up(slots * max(plan.rows - SUB, 0) + 2 * SUB, SUB)
    carried = [(slots, 4, deep, LANES), (slots, SUB, LANES)]
    ends = stage == plan.chips
    outs = [(slots, LANES)] if ends else carried
    scratch = (carried if ends else []) + [(fresh, 4, g, deep, LANES), (4, long, LANES), (long, LANES)]
    return pl.pallas_call(
        functools.partial(cost_kernel, plan, stage),
        out_shape=[jax.ShapeDtypeStruct(shape, jnp.float32) for shape in outs],
        in_specs=[VMEM] * (len(chunks) + len(before)),
        out_specs=[VMEM] * len(outs),
        scratch_shapes=[pltpu.VMEM(shape, jnp.float32) for shape in scratch]
        + [pltpu.SMEM((slots,), jnp.int32), pltpu.SMEM((fresh,), jnp.int32)],
        compiler_params=PARAMS,
        cost_estimate=pl.CostEstimate(
            flops=10_000_000 * (stage + 1), bytes_accessed=1000, transcendentals=0
        ),
        name=f"cost{stage}",
    )(*chunks, *before)


def owner_kernel(plan, costs, out):
    for l in range(plan.here):
        for t in range(plan.tiles):
            out[l : l + 1, t * LANES : (t + 1) * LANES] = owned(plan, costs, l, t)


def owned(plan, costs, l, t):
    here, g = plan.here, plan.lane_groups
    line = costs[t * g * here + l : t * g * here + l + 1, :]
    for d in range(t * g + 1, (t + 1) * g):
        line = line + costs[d * here + l : d * here + l + 1, :]
    return line


def owner(plan, costs):
    return pl.pallas_call(
        functools.partial(owner_kernel, plan),
        out_shape=jax.ShapeDtypeStruct((plan.here, plan.columns), jnp.float32),
        in_specs=[VMEM],
        out_specs=VMEM,
        compiler_params=PARAMS,
        cost_estimate=pl.CostEstimate(flops=4_000_000, bytes_accessed=1000, transcendentals=0),
        name="owner",
    )(costs)


def blend_kernel(plan, seeds_here, costs, stored, sums):
    n, here = plan.spheres, plan.here
    n_rows = n // 4
    step = plan.tiles * here
    seed_of = iota((seeds_here, LANES), 1) // W
    seed = iota((seeds_here, LANES), 0)
    fold = iota((n_rows, LANES), 1) // W
    per_tile = LANES // W
    for l in range(here):
        seed_cost = jnp.zeros((seeds_here, 1), jnp.float32)
        for t in range(plan.tiles):
            line = owned(plan, costs, l, t)
            mine = seed_of + t * per_tile == seed
            seed_cost = seed_cost + jnp.sum(jnp.where(mine, line, 0.0), axis=1, keepdims=True)
        weight = 1.0 / (1.0 + seed_cost)
        spread = []
        for t in range(plan.tiles):
            mine = seed_of + t * per_tile == seed
            spread.append(jnp.sum(jnp.where(mine, weight, 0.0), axis=0, keepdims=True))
        total = jnp.sum(weight, axis=0, keepdims=True)
        sums[here * 3 * n_rows + l : here * 3 * n_rows + l + 1, :] = jnp.broadcast_to(total, (1, LANES))
        for c in range(3):
            pieces = []
            for j in range(4):
                x = jnp.zeros((n_rows, LANES), jnp.float32)
                for t in range(plan.tiles):
                    at = (c * n + j) * step + t * here + l
                    x = x + stored[pl.ds(at, n_rows, stride=4 * step), :] * spread[t]
                pieces.append(x)
            y = jnp.zeros((n_rows, LANES), jnp.float32)
            for turn in range(4):
                z = pieces[0]
                for j in range(4):
                    z = jnp.where(fold == (j - turn) % 4, pieces[j], z)
                y = y + (pltpu.roll(z, turn * W, 1) if turn else z)
            at = (l * 3 + c) * n_rows
            sums[at : at + n_rows, :] = y


def blend(plan, costs, stored):
    seeds_here = plan.columns // W
    rows = round_up(plan.here * (3 * plan.spheres // 4 + 1), SUB)
    return pl.pallas_call(
        functools.partial(blend_kernel, plan, seeds_here),
        out_shape=jax.ShapeDtypeStruct((rows, LANES), jnp.float32),
        in_specs=[VMEM, VMEM],
        out_specs=VMEM,
        compiler_params=PARAMS,
        name="blend",
    )(costs, stored)


def finish_kernel(plan, *refs):
    parts, out, wide = refs[:-2], refs[-2], refs[-1]
    n_rows = plan.spheres // 4
    for l in range(plan.here):
        at = plan.here * 3 * n_rows + l
        total = parts[0][at : at + 1, :]
        for p in parts[1:]:
            total = total + p[at : at + 1, :]
        inverse = 1.0 / total
        for c in range(3):
            at = (l * 3 + c) * n_rows
            y = parts[0][at : at + n_rows, :]
            for p in parts[1:]:
                y = y + p[at : at + n_rows, :]
            y = y * inverse
            for j in range(4):
                z = pltpu.roll(y, (LANES - j * W) % LANES, 1) if j else y
                wide[l * 3 + c, pl.ds(j, n_rows, stride=4), :] = z
            out[l, c] = wide[l * 3 + c].T[:W]


def finish(plan, parts):
    return pl.pallas_call(
        functools.partial(finish_kernel, plan),
        out_shape=jax.ShapeDtypeStruct((plan.here, 3, W, plan.spheres), jnp.float32),
        in_specs=[VMEM] * len(parts),
        out_specs=VMEM,
        scratch_shapes=[pltpu.VMEM((plan.here * 3, plan.spheres, LANES), jnp.float32)],
        compiler_params=PARAMS,
        name="finish",
    )(*parts)


def exchanged(block, axis, k):
    size = lax.axis_size(axis)
    return lax.ppermute(block, axis, [(i, i ^ k) for i in range(size)])


def local(centres, sphere_radius, counts, adjacency):
    here, _, spheres, columns = centres.shape
    plan = Plan(lax.axis_size("robot"), here, spheres, columns)
    stored = centres.reshape(here, 3, spheres, plan.tiles, LANES)
    stored = stored.transpose(1, 2, 3, 0, 4).reshape(-1, LANES)
    theirs, stored, lines = pack(plan, 1, stored, counts.reshape(1, -1), sphere_radius, adjacency)
    theirs = exchanged(theirs, "robot", 1)
    (mine,) = pack(plan, 0, lines, stored)
    carried = cost(plan, 0, [mine], [])
    mine, *carried = lax.optimization_barrier((mine, *carried))
    chunks = [mine, theirs]
    for k, pair in enumerate(join(plan, mine, theirs), 1):
        chunks.append(exchanged(pair, "robot", 2 * k))
    for stage in range(1, plan.chips + 1):
        carried = cost(plan, stage, chunks[: stage + 1], carried)
    (costs,) = carried
    costs = lax.all_to_all(costs, "robot", 0, 0, tiled=True)
    sums = blend(plan, costs, stored)
    parts = [sums] + [exchanged(sums, "seed", k) for k in range(1, lax.axis_size("seed"))]
    return owner(plan, costs), finish(plan, parts).transpose(0, 1, 3, 2)


def solution(mesh):
    return jax.shard_map(
        local,
        mesh=mesh,
        in_specs=(P("robot", None, None, "seed"), P("robot", None), P("robot"), P("robot", None)),
        out_specs=(P("robot", "seed"), P("robot", None, None, None)),
        check_vma=False,
    )
```

```python
import functools
import math

import jax
import jax.numpy as jnp
from jax import lax
from jax.experimental import pallas as pl
from jax.experimental.pallas import tpu as pltpu
from jax.sharding import PartitionSpec as P

W = 32
LANES = 128
SUB = 8
SCALE = math.sqrt(math.log2(math.e))
FAR = 1e15
COUNTS = 64
VMEM = pl.BlockSpec(memory_space=pltpu.VMEM)
SMEM = pl.BlockSpec(memory_space=pltpu.SMEM)
PARAMS = pltpu.CompilerParams(vmem_limit_bytes=16 * 1024 * 1024)


def round_up(value, step):
    return -(-value // step) * step


class Plan:
    def __init__(self, group, robots_here, spheres, columns):
        self.group = group
        self.chips = group // 2
        self.here = robots_here
        self.spheres = spheres
        self.columns = columns
        self.width = columns // group
        self.lane_groups = LANES // self.width
        self.rows = -(-spheres // self.lane_groups)
        self.padded = self.rows * self.lane_groups
        self.parts = -(-self.rows // SUB)
        self.slots = group * robots_here
        self.halves = -(-self.slots // 16)
        self.sweep_late = self.width % W == 0
        self.fields = 3 if self.sweep_late else 4
        self.data_rows = robots_here * self.fields * self.rows
        self.chunk_rows = round_up(self.data_rows + robots_here, SUB)
        self.tiles = columns // LANES

    def arrival(self, stage):
        k = stage if stage < 2 else 2 * (stage - 1)
        return k * self.here, self.here if stage < 2 else 2 * self.here


def iota(shape, axis):
    return lax.broadcasted_iota(jnp.int32, shape, axis)


def sweep(points, last, radius):
    squares = None
    middles = []
    for x in points:
        ahead = jnp.where(last, x, pltpu.roll(x, LANES - 1, 1))
        middles.append((0.5 * SCALE) * (x + ahead))
        square = (ahead - x) * (ahead - x)
        squares = square if squares is None else squares + square
    return middles, radius + 0.5 * jnp.sqrt(squares + 1e-06)


def fetch(plan, sources, stored, lines, counts, radius, adjacency, sem):
    n = plan.spheres
    copies = [
        pltpu.make_async_copy(src, dst, sem.at[i])
        for i, (src, dst) in enumerate(zip(sources, (stored, counts, radius, adjacency)))
    ]
    for copy in copies:
        copy.start()
    for copy in copies[1:]:
        copy.wait()
    lane = iota((1, LANES), 1)
    links = iota((1, plan.slots), 1)
    for l in range(plan.here):
        head = jnp.zeros((1, LANES), jnp.float32)
        for h in range(plan.halves):
            bits = jnp.where(
                (adjacency[l : l + 1, :] != 0) & (links // 16 == h), 1 << (links % 16), 0
            )
            value = jnp.sum(bits.astype(jnp.float32), axis=1, keepdims=True)
            if h == 0:
                value = value * COUNTS + counts[:, l : l + 1].astype(jnp.float32)
            head = jnp.where(lane == n + h, value, head)
        lines[l : l + 1, :] = head
        lines[l : l + 1, 0:n] = radius[l : l + 1, :]
    copies[0].wait()


def pack_kernel(plan, core, *refs):
    if core:
        out, stored, lines, source = refs[4:8]
        fetch(plan, refs[:4], stored, lines, *refs[8:])
    else:
        lines, stored, out, source = refs
    me = lax.axis_index("robot")
    n, g, rows, width, here = plan.spheres, plan.lane_groups, plan.rows, plan.width, plan.here
    step = plan.tiles * here
    if not plan.sweep_late:
        order = iota((n, LANES), 0)
        diagonal = iota((n, n), 0) == iota((n, n), 1)
        for l in range(here):
            column = jnp.sum(jnp.where(diagonal, lines[l : l + 1, 0:n], 0.0), axis=1, keepdims=True)
            count = lines[l : l + 1, n : n + 1].astype(jnp.int32) % COUNTS
            robot = me * here + l
            off = FAR * (1 + order + plan.padded * robot).astype(jnp.float32)
            for t in range(plan.tiles):
                points = [
                    stored[pl.ds(c * n * step + t * here + l, n, stride=step), :] for c in range(3)
                ]
                fields, swept = sweep(points, iota((n, LANES), 1) % W == W - 1, column)
                fields[0] = jnp.where(order < count, fields[0], off)
                for c, x in enumerate(fields + [swept]):
                    source[t, l * 4 + c, 0:n, :] = x
                if plan.padded > n:
                    index = n + iota((plan.padded - n, LANES), 0) + plan.padded * robot
                    fill = FAR * (1 + index).astype(jnp.float32)
                    for c in range(4):
                        source[t, l * 4 + c, n:, :] = fill if c == 0 else jnp.ones_like(fill)
    lane_group = iota((rows, LANES), 1) // width
    for k in range(plan.chips):
        dest = me ^ (2 * k + core)
        tile = dest // g
        spot = dest % g
        for l in range(here):
            for c in range(plan.fields):
                y = jnp.zeros((rows, LANES), jnp.float32)
                for j in range(g):
                    if plan.sweep_late:
                        at = (c * n + j) * step + tile * here + l
                        x = stored[pl.ds(at, rows, stride=g * step), :]
                    else:
                        x = source[tile, l * 4 + c, pl.ds(j, rows, stride=g), :]
                    x = pltpu.roll(x, ((j + g - spot) % g) * width, 1)
                    y = jnp.where(lane_group == j, x, y)
                at = (l * plan.fields + c) * rows
                out[k, at : at + rows, :] = y
            at = plan.data_rows + l
            out[k, at : at + 1, :] = lines[l : l + 1, :]


def pack(plan, core, *args):
    shapes = [(plan.chips, plan.chunk_rows, LANES)]
    swept = (plan.tiles, plan.here * 4, plan.padded, LANES)
    scratch = [pltpu.VMEM((SUB, LANES) if plan.sweep_late else swept, jnp.float32)]
    specs = [VMEM, VMEM]
    if core:
        shapes += [args[0].shape, (plan.here, LANES)]
        scratch += [pltpu.VMEM(x.shape, x.dtype) for x in args[1:]]
        scratch += [pltpu.SemaphoreType.DMA((len(args),))]
        specs = [pl.BlockSpec(memory_space=pltpu.HBM)] * len(args)
        args = [pltpu.with_memory_space_constraint(x, pltpu.HBM) for x in args]
    return pl.pallas_call(
        functools.partial(pack_kernel, plan, core),
        out_shape=[jax.ShapeDtypeStruct(shape, jnp.float32) for shape in shapes],
        in_specs=specs,
        out_specs=[VMEM] * len(shapes),
        scratch_shapes=scratch,
        compiler_params=PARAMS,
        cost_estimate=pl.CostEstimate(flops=4_000_000, bytes_accessed=1000, transcendentals=0),
        name=f"pack{core}",
    )(*args)


def join_kernel(plan, mine, theirs, *outs):
    for k in range(1, plan.chips):
        outs[k - 1][0] = mine[k]
        outs[k - 1][1] = theirs[k]


def join(plan, mine, theirs):
    pair = jax.ShapeDtypeStruct((2, plan.chunk_rows, LANES), jnp.float32)
    return pl.pallas_call(
        functools.partial(join_kernel, plan),
        out_shape=[pair] * (plan.chips - 1),
        in_specs=[VMEM, VMEM],
        out_specs=[VMEM] * (plan.chips - 1),
        compiler_params=PARAMS,
        name="join",
    )(mine, theirs)


def term(first, second):
    gap = first[0] - second[0]
    square = gap * gap
    for c in (1, 2):
        gap = first[c] - second[c]
        square = square + gap * gap
    inverse = 1.0 / (first[3] + second[3])
    return jnp.exp2(-(square * (inverse * inverse)))


def masked(value, keep):
    return value if keep is None else jnp.where(keep, value, 0.0)


def cost_kernel(plan, stage, *refs):
    chunks, refs = refs[: stage + 1], refs[stage + 1 :]
    before, refs = refs[: 2 if stage else 0], refs[2 if stage else 0 :]
    ends = stage == plan.chips
    if ends:
        out, store, totals, blocks, tails, sums, starts, links = refs
    else:
        store, totals, blocks, tails, sums, starts, links = refs
    me = lax.axis_index("robot")
    g, rows, width, here, n = plan.lane_groups, plan.rows, plan.width, plan.here, plan.spheres
    parts = plan.parts
    first_slot, fresh = plan.arrival(stage)
    deep = parts * SUB

    def chunk_of(slot):
        k = slot // here
        return chunks[k].at[0] if k < 2 else chunks[k // 2 + 1].at[k % 2]

    def line_of(slot):
        at = plan.data_rows + slot % here
        return chunk_of(slot)[at : at + 1, :]

    per_word = 8
    words = []
    if parts > 1:
        for at in range(0, first_slot, per_word):
            word = before[1][first_slot, 0:1, :][0, at // per_word].astype(jnp.int32)
            words.append(word)
            for u in range(at, min(at + per_word, first_slot)):
                starts[u] = SUB + ((word >> (3 * (u - at))) & 7)
    for i in range(fresh):
        slot = first_slot + i
        line = line_of(slot)
        bits = line[0, n].astype(jnp.int32)
        count = bits % COUNTS
        bits = bits // COUNTS
        for h in range(1, plan.halves):
            bits = bits | (line[0, n + h].astype(jnp.int32) << (16 * h))
        filled = jnp.minimum((count + g - 1) // g, rows)
        starts[slot] = filled
        if parts > 1:
            if slot % per_word == 0:
                words.append(jnp.int32(0))
            more = jnp.maximum(filled - SUB, 0)
            words[-1] = words[-1] + (more << (3 * (slot % per_word)))
        step = 1
        while step < plan.slots:
            low = sum(1 << b for b in range(plan.slots) if not b & step)
            low = low - (1 << 32) if low >= 1 << 31 else low
            turned = ((bits & low) << step) | ((bits >> step) & low)
            bits = jnp.where((me * here) & step != 0, turned, bits)
            step *= 2
        links[i] = bits & ((1 << (first_slot + i)) - 1)

    sphere = iota((rows, LANES), 0) * g + iota((rows, LANES), 1) // width
    last = iota((rows, LANES), 1) % W == W - 1
    for i in range(fresh):
        slot = first_slot + i
        chunk = chunk_of(slot)
        at = slot % here * plan.fields * rows
        fields = [chunk[at + f * rows : at + (f + 1) * rows, :] for f in range(plan.fields)]
        if plan.sweep_late:
            line = line_of(slot)
            wide = jnp.broadcast_to(line, (SUB, LANES))
            pick = iota((SUB, LANES), 0) * g + iota((SUB, LANES), 1) // width
            radius = [
                jnp.take_along_axis(
                    wide, jnp.minimum(pick + p * SUB * g, LANES - 1), axis=1,
                    mode="promise_in_bounds",
                )
                for p in range(parts)
            ]
            fields, swept = sweep(fields, last, jnp.concatenate(radius, axis=0)[:rows])
            count = line[:, n : n + 1].astype(jnp.int32) % COUNTS
            off = FAR * (1 + sphere + plan.padded * slot).astype(jnp.float32)
            fields[0] = jnp.where(sphere < count, fields[0], off)
            fields.append(swept)
        for c in range(4):
            x = fields[c]
            for m in range(1, g):
                blocks[i, c, m, 0:rows, :] = pltpu.roll(x, m * width, 1)
            store[slot, c, 0:rows, :] = x
            if deep > rows:
                fill = jnp.full((deep - rows, LANES), -FAR if c == 0 else 1.0, jnp.float32)
                store[slot, c, rows:deep, :] = fill
        totals[slot] = jnp.zeros((SUB, LANES), jnp.float32)
    for u in range(first_slot):
        store[u] = before[0][u]
        totals[u] = before[1][u]
    if parts > 1 and not ends:
        lane = iota((SUB, LANES), 1)
        line = jnp.zeros((SUB, LANES), jnp.float32)
        for at, word in enumerate(words):
            line = jnp.where(lane == at, word.astype(jnp.float32), line)
        totals[first_slot + fresh] = line

    def row(i, m, r):
        if m == 0:
            return [store[first_slot + i, c, r : r + 1, :] for c in range(4)]
        return [blocks[i, c, m, r : r + 1, :] for c in range(4)]

    def part(slot, p):
        return [store[slot, c, p * SUB : (p + 1) * SUB, :] for c in range(4)]

    sub = iota((SUB, LANES), 0)
    lane_group = iota((SUB, LANES), 1) // width
    nothing = jnp.zeros((SUB, LANES), jnp.float32)

    def self_terms(u, high):
        total = nothing
        second = part(first_slot + u, 0)
        for d in range(SUB // 2 + 1):
            turned = [pltpu.roll(x, SUB - d, 0) for x in second] if d else second
            low = (sub + d) % SUB
            for m in range(g):
                other = (lane_group + g - m) % g
                if d == 0:
                    if m < 2:
                        continue
                    keep = lane_group >= m
                elif d == 1 and m == 1:
                    keep = jnp.abs((low - sub) * g + lane_group - other) >= 2
                elif 2 * d == SUB:
                    keep = sub < d
                else:
                    keep = None
                first = [blocks[u, c, m, 0:SUB, :] for c in range(4)] if m else second
                total = total + masked(term(first, turned), keep)
        for r in range(SUB, high):
            for p in range(parts):
                if p * SUB > r:
                    continue
                second = part(first_slot + u, p)
                for m in range(g):
                    other = (lane_group + g - m) % g
                    ahead = (r - p * SUB - sub) * g + other - lane_group
                    near = r < (p + 1) * SUB + 1
                    total = total + masked(term(row(u, m, r), second), ahead >= 2 if near else None)
        return total

    def against(u, high, second):
        value = nothing
        for r in range(high):
            for m in range(g):
                value = value + term(row(u, m, r), second)
        return value

    def lowest_bit(bits):
        return 31 - lax.clz(bits & -bits)

    def with_rows(u, high):
        total = self_terms(u, high)

        def neighbour(state):
            bits, filled, total = state
            v = lowest_bit(bits)
            value = against(u, high, part(v, 0))
            totals[v] = totals[v] + value
            if parts > 1:
                for c, x in enumerate(part(v, 1)):
                    tails[c, pl.ds(filled, SUB), :] = x
                filled = filled + jnp.maximum(starts[v] - SUB, 0)
            return bits & (bits - 1), filled, total + value

        state = (links[u], jnp.int32(0), total)
        _, filled, total = lax.while_loop(lambda state: state[0] != 0, neighbour, state)
        if parts > 1:
            for c in range(4):
                fill = jnp.full((SUB, LANES), -FAR if c == 0 else 1.0, jnp.float32)
                tails[c, pl.ds(filled, SUB), :] = fill

            def trip(j, total):
                at = pl.multiple_of(j * SUB, SUB)
                value = against(u, high, [tails[c, pl.ds(at, SUB), :] for c in range(4)])
                sums[pl.ds(at, SUB), :] = value
                return total + value

            total = lax.fori_loop(0, (filled + SUB - 1) // SUB, trip, total)
        totals[first_slot + u] = totals[first_slot + u] + total

    lowest = max(1, -(-(n // 2) // g))

    def choose(u, low, high):
        if low == high:
            with_rows(u, high)
            return
        middle = (low + high) // 2

        @pl.when(starts[first_slot + u] <= middle)
        def _():
            choose(u, low, middle)

        @pl.when(starts[first_slot + u] > middle)
        def _():
            choose(u, middle + 1, high)

    @pl.loop(0, fresh)
    def _(u):
        choose(u, lowest, rows)
        if parts > 1:

            def hand_out(state):
                bits, filled = state
                v = lowest_bit(bits)
                more = jnp.maximum(starts[v] - SUB, 0)
                totals[v] = totals[v] + jnp.where(sub < more, sums[pl.ds(filled, SUB), :], 0.0)
                return bits & (bits - 1), filled + more

            lax.while_loop(lambda state: state[0] != 0, hand_out, (links[u], jnp.int32(0)))

    if not ends:
        return
    spot = iota((1, LANES), 1) // width == me % g
    for k in range(plan.group):
        for l in range(here):
            value = jnp.sum(totals[k * here + l], axis=0, keepdims=True)
            value = sum([pltpu.roll(value, m * width, 1) for m in range(1, g)], value)
            value = jnp.where(spot, value, 0.0) / (n * n)
            out[pl.ds((me ^ k) * here + l, 1), :] = value


def cost(plan, stage, chunks, before):
    first_slot, fresh = plan.arrival(stage)
    slots, g = first_slot + fresh, plan.lane_groups
    deep = plan.parts * SUB
    long = round_up(slots * max(plan.rows - SUB, 0) + 2 * SUB, SUB)
    carried = [(slots, 4, deep, LANES), (slots + 1, SUB, LANES)]
    ends = stage == plan.chips
    outs = [(slots, LANES)] if ends else carried
    scratch = (carried if ends else []) + [(fresh, 4, g, deep, LANES), (4, long, LANES), (long, LANES)]
    return pl.pallas_call(
        functools.partial(cost_kernel, plan, stage),
        out_shape=[jax.ShapeDtypeStruct(shape, jnp.float32) for shape in outs],
        in_specs=[VMEM] * (len(chunks) + len(before)),
        out_specs=[VMEM] * len(outs),
        scratch_shapes=[pltpu.VMEM(shape, jnp.float32) for shape in scratch]
        + [pltpu.SMEM((slots,), jnp.int32), pltpu.SMEM((fresh,), jnp.int32)],
        compiler_params=PARAMS,
        cost_estimate=pl.CostEstimate(
            flops=10_000_000 * (stage + 1), bytes_accessed=1000, transcendentals=0
        ),
        name=f"cost{stage}",
    )(*chunks, *before)


def owner_kernel(plan, costs, out):
    for l in range(plan.here):
        for t in range(plan.tiles):
            out[l : l + 1, t * LANES : (t + 1) * LANES] = owned(plan, costs, l, t)


def owned(plan, costs, l, t):
    here, g = plan.here, plan.lane_groups
    line = costs[t * g * here + l : t * g * here + l + 1, :]
    for d in range(t * g + 1, (t + 1) * g):
        line = line + costs[d * here + l : d * here + l + 1, :]
    return line


def owner(plan, costs):
    return pl.pallas_call(
        functools.partial(owner_kernel, plan),
        out_shape=jax.ShapeDtypeStruct((plan.here, plan.columns), jnp.float32),
        in_specs=[VMEM],
        out_specs=VMEM,
        compiler_params=PARAMS,
        cost_estimate=pl.CostEstimate(flops=4_000_000, bytes_accessed=1000, transcendentals=0),
        name="owner",
    )(costs)


def blend_kernel(plan, seeds_here, costs, stored, sums):
    n, here = plan.spheres, plan.here
    n_rows = n // 4
    step = plan.tiles * here
    seed_of = iota((seeds_here, LANES), 1) // W
    seed = iota((seeds_here, LANES), 0)
    fold = iota((n_rows, LANES), 1) // W
    per_tile = LANES // W
    for l in range(here):
        seed_cost = jnp.zeros((seeds_here, 1), jnp.float32)
        for t in range(plan.tiles):
            line = owned(plan, costs, l, t)
            mine = seed_of + t * per_tile == seed
            seed_cost = seed_cost + jnp.sum(jnp.where(mine, line, 0.0), axis=1, keepdims=True)
        weight = 1.0 / (1.0 + seed_cost)
        spread = []
        for t in range(plan.tiles):
            mine = seed_of + t * per_tile == seed
            spread.append(jnp.sum(jnp.where(mine, weight, 0.0), axis=0, keepdims=True))
        total = jnp.sum(weight, axis=0, keepdims=True)
        sums[here * 3 * n_rows + l : here * 3 * n_rows + l + 1, :] = jnp.broadcast_to(total, (1, LANES))
        for c in range(3):
            pieces = []
            for j in range(4):
                x = jnp.zeros((n_rows, LANES), jnp.float32)
                for t in range(plan.tiles):
                    at = (c * n + j) * step + t * here + l
                    x = x + stored[pl.ds(at, n_rows, stride=4 * step), :] * spread[t]
                pieces.append(x)
            y = jnp.zeros((n_rows, LANES), jnp.float32)
            for turn in range(4):
                z = pieces[0]
                for j in range(4):
                    z = jnp.where(fold == (j - turn) % 4, pieces[j], z)
                y = y + (pltpu.roll(z, turn * W, 1) if turn else z)
            at = (l * 3 + c) * n_rows
            sums[at : at + n_rows, :] = y


def blend(plan, costs, stored):
    seeds_here = plan.columns // W
    rows = round_up(plan.here * (3 * plan.spheres // 4 + 1), SUB)
    return pl.pallas_call(
        functools.partial(blend_kernel, plan, seeds_here),
        out_shape=jax.ShapeDtypeStruct((rows, LANES), jnp.float32),
        in_specs=[VMEM, VMEM],
        out_specs=VMEM,
        compiler_params=PARAMS,
        name="blend",
    )(costs, stored)


def finish_kernel(plan, *refs):
    parts, out, wide = refs[:-2], refs[-2], refs[-1]
    n_rows = plan.spheres // 4
    for l in range(plan.here):
        at = plan.here * 3 * n_rows + l
        total = parts[0][at : at + 1, :]
        for p in parts[1:]:
            total = total + p[at : at + 1, :]
        inverse = 1.0 / total
        for c in range(3):
            at = (l * 3 + c) * n_rows
            y = parts[0][at : at + n_rows, :]
            for p in parts[1:]:
                y = y + p[at : at + n_rows, :]
            y = y * inverse
            for j in range(4):
                z = pltpu.roll(y, (LANES - j * W) % LANES, 1) if j else y
                wide[l * 3 + c, pl.ds(j, n_rows, stride=4), :] = z
            out[l, c] = wide[l * 3 + c].T[:W]


def finish(plan, parts):
    return pl.pallas_call(
        functools.partial(finish_kernel, plan),
        out_shape=jax.ShapeDtypeStruct((plan.here, 3, W, plan.spheres), jnp.float32),
        in_specs=[VMEM] * len(parts),
        out_specs=VMEM,
        scratch_shapes=[pltpu.VMEM((plan.here * 3, plan.spheres, LANES), jnp.float32)],
        compiler_params=PARAMS,
        name="finish",
    )(*parts)


def exchanged(block, axis, k):
    size = lax.axis_size(axis)
    return lax.ppermute(block, axis, [(i, i ^ k) for i in range(size)])


def local(centres, sphere_radius, counts, adjacency):
    here, _, spheres, columns = centres.shape
    plan = Plan(lax.axis_size("robot"), here, spheres, columns)
    stored = centres.reshape(here, 3, spheres, plan.tiles, LANES)
    stored = stored.transpose(1, 2, 3, 0, 4).reshape(-1, LANES)
    theirs, stored, lines = pack(plan, 1, stored, counts.reshape(1, -1), sphere_radius, adjacency)
    theirs = exchanged(theirs, "robot", 1)
    (mine,) = pack(plan, 0, lines, stored)
    carried = cost(plan, 0, [mine], [])
    mine, *carried = lax.optimization_barrier((mine, *carried))
    chunks = [mine, theirs]
    for k, pair in enumerate(join(plan, mine, theirs), 1):
        chunks.append(exchanged(pair, "robot", 2 * k))
    for stage in range(1, plan.chips + 1):
        carried = cost(plan, stage, chunks[: stage + 1], carried)
    (costs,) = carried
    costs = lax.all_to_all(costs, "robot", 0, 0, tiled=True)
    sums = blend(plan, costs, stored)
    parts = [sums] + [exchanged(sums, "seed", k) for k in range(1, lax.axis_size("seed"))]
    return owner(plan, costs), finish(plan, parts).transpose(0, 1, 3, 2)


def solution(mesh):
    return jax.shard_map(
        local,
        mesh=mesh,
        in_specs=(P("robot", None, None, "seed"), P("robot", None), P("robot"), P("robot", None)),
        out_specs=(P("robot", "seed"), P("robot", None, None, None)),
        check_vma=False,
    )
```

```python
import functools
import math

import jax
import jax.numpy as jnp
from jax import lax
from jax.experimental import pallas as pl
from jax.experimental.pallas import tpu as pltpu
from jax.sharding import PartitionSpec as P

W = 32
LANES = 128
SUB = 8
SCALE = math.sqrt(math.log2(math.e))
FAR = 1e15
COUNTS = 64
VMEM = pl.BlockSpec(memory_space=pltpu.VMEM)
SMEM = pl.BlockSpec(memory_space=pltpu.SMEM)
PARAMS = pltpu.CompilerParams(vmem_limit_bytes=16 * 1024 * 1024)


def round_up(value, step):
    return -(-value // step) * step


class Plan:
    def __init__(self, group, robots_here, spheres, columns):
        self.group = group
        self.chips = group // 2
        self.here = robots_here
        self.spheres = spheres
        self.columns = columns
        self.width = columns // group
        self.lane_groups = LANES // self.width
        self.rows = -(-spheres // self.lane_groups)
        self.padded = self.rows * self.lane_groups
        self.parts = -(-self.rows // SUB)
        self.slots = group * robots_here
        self.halves = -(-self.slots // 16)
        self.sweep_late = self.width % W == 0
        self.fields = 3 if self.sweep_late else 4
        self.data_rows = robots_here * self.fields * self.rows
        self.chunk_rows = round_up(self.data_rows + robots_here, SUB)
        self.tiles = columns // LANES

    def arrival(self, stage):
        k = stage if stage < 2 else 2 * (stage - 1)
        return k * self.here, self.here if stage < 2 else 2 * self.here


def iota(shape, axis):
    return lax.broadcasted_iota(jnp.int32, shape, axis)


def sweep(points, last, radius):
    squares = None
    middles = []
    for x in points:
        ahead = jnp.where(last, x, pltpu.roll(x, LANES - 1, 1))
        middles.append((0.5 * SCALE) * (x + ahead))
        square = (ahead - x) * (ahead - x)
        squares = square if squares is None else squares + square
    return middles, radius + 0.5 * jnp.sqrt(squares + 1e-06)


def fetch(plan, sources, stored, lines, counts, radius, adjacency, sem):
    n = plan.spheres
    copies = [
        pltpu.make_async_copy(src, dst, sem.at[i])
        for i, (src, dst) in enumerate(zip(sources, (stored, counts, radius, adjacency)))
    ]
    for copy in copies:
        copy.start()
    for copy in copies[1:]:
        copy.wait()
    lane = iota((1, LANES), 1)
    links = iota((1, plan.slots), 1)
    for l in range(plan.here):
        head = jnp.zeros((1, LANES), jnp.float32)
        for h in range(plan.halves):
            bits = jnp.where(
                (adjacency[l : l + 1, :] != 0) & (links // 16 == h), 1 << (links % 16), 0
            )
            value = jnp.sum(bits.astype(jnp.float32), axis=1, keepdims=True)
            if h == 0:
                value = value * COUNTS + counts[:, l : l + 1].astype(jnp.float32)
            head = jnp.where(lane == n + h, value, head)
        lines[l : l + 1, :] = head
        lines[l : l + 1, 0:n] = radius[l : l + 1, :]
    copies[0].wait()


def pack_kernel(plan, core, *refs):
    if core:
        out, stored, lines, source = refs[4:8]
        fetch(plan, refs[:4], stored, lines, *refs[8:])
    else:
        lines, stored, out, source = refs
    me = lax.axis_index("robot")
    n, g, rows, width, here = plan.spheres, plan.lane_groups, plan.rows, plan.width, plan.here
    step = plan.tiles * here
    if not plan.sweep_late:
        order = iota((n, LANES), 0)
        diagonal = iota((n, n), 0) == iota((n, n), 1)
        for l in range(here):
            column = jnp.sum(jnp.where(diagonal, lines[l : l + 1, 0:n], 0.0), axis=1, keepdims=True)
            count = lines[l : l + 1, n : n + 1].astype(jnp.int32) % COUNTS
            robot = me * here + l
            off = FAR * (1 + order + plan.padded * robot).astype(jnp.float32)
            for t in range(plan.tiles):
                points = [
                    stored[pl.ds(c * n * step + t * here + l, n, stride=step), :] for c in range(3)
                ]
                fields, swept = sweep(points, iota((n, LANES), 1) % W == W - 1, column)
                fields[0] = jnp.where(order < count, fields[0], off)
                for c, x in enumerate(fields + [swept]):
                    source[t, l * 4 + c, 0:n, :] = x
                if plan.padded > n:
                    index = n + iota((plan.padded - n, LANES), 0) + plan.padded * robot
                    fill = FAR * (1 + index).astype(jnp.float32)
                    for c in range(4):
                        source[t, l * 4 + c, n:, :] = fill if c == 0 else jnp.ones_like(fill)
    lane_group = iota((rows, LANES), 1) // width
    for k in range(plan.chips):
        dest = me ^ (2 * k + core)
        tile = dest // g
        spot = dest % g
        for l in range(here):
            for c in range(plan.fields):
                y = jnp.zeros((rows, LANES), jnp.float32)
                for j in range(g):
                    if plan.sweep_late:
                        at = (c * n + j) * step + tile * here + l
                        x = stored[pl.ds(at, rows, stride=g * step), :]
                    else:
                        x = source[tile, l * 4 + c, pl.ds(j, rows, stride=g), :]
                    x = pltpu.roll(x, ((j + g - spot) % g) * width, 1)
                    y = jnp.where(lane_group == j, x, y)
                at = (l * plan.fields + c) * rows
                out[k, at : at + rows, :] = y
            at = plan.data_rows + l
            out[k, at : at + 1, :] = lines[l : l + 1, :]


def pack(plan, core, *args):
    shapes = [(plan.chips, plan.chunk_rows, LANES)]
    swept = (plan.tiles, plan.here * 4, plan.padded, LANES)
    scratch = [pltpu.VMEM((SUB, LANES) if plan.sweep_late else swept, jnp.float32)]
    specs = [VMEM, VMEM]
    if core:
        shapes += [args[0].shape, (plan.here, LANES)]
        scratch += [pltpu.VMEM(x.shape, x.dtype) for x in args[1:]]
        scratch += [pltpu.SemaphoreType.DMA((len(args),))]
        specs = [pl.BlockSpec(memory_space=pltpu.HBM)] * len(args)
        args = [pltpu.with_memory_space_constraint(x, pltpu.HBM) for x in args]
    return pl.pallas_call(
        functools.partial(pack_kernel, plan, core),
        out_shape=[jax.ShapeDtypeStruct(shape, jnp.float32) for shape in shapes],
        in_specs=specs,
        out_specs=[VMEM] * len(shapes),
        scratch_shapes=scratch,
        compiler_params=PARAMS,
        cost_estimate=pl.CostEstimate(flops=4_000_000, bytes_accessed=1000, transcendentals=0),
        name=f"pack{core}",
    )(*args)


def join_kernel(plan, mine, theirs, *outs):
    for k in range(1, plan.chips):
        outs[k - 1][0] = mine[k]
        outs[k - 1][1] = theirs[k]


def join(plan, mine, theirs):
    pair = jax.ShapeDtypeStruct((2, plan.chunk_rows, LANES), jnp.float32)
    return pl.pallas_call(
        functools.partial(join_kernel, plan),
        out_shape=[pair] * (plan.chips - 1),
        in_specs=[VMEM, VMEM],
        out_specs=[VMEM] * (plan.chips - 1),
        compiler_params=PARAMS,
        name="join",
    )(mine, theirs)


def term(first, second):
    gap = first[0] - second[0]
    square = gap * gap
    for c in (1, 2):
        gap = first[c] - second[c]
        square = square + gap * gap
    inverse = 1.0 / (first[3] + second[3])
    return jnp.exp2(-(square * (inverse * inverse)))


def masked(value, keep):
    return value if keep is None else jnp.where(keep, value, 0.0)


def cost_kernel(plan, stage, *refs):
    chunks, refs = refs[: stage + 1], refs[stage + 1 :]
    before, refs = refs[: 2 if stage else 0], refs[2 if stage else 0 :]
    ends = stage == plan.chips
    if ends:
        out, store, totals, blocks, tails, sums, starts, links = refs
    else:
        store, totals, blocks, tails, sums, starts, links = refs
    me = lax.axis_index("robot")
    g, rows, width, here, n = plan.lane_groups, plan.rows, plan.width, plan.here, plan.spheres
    parts = plan.parts
    first_slot, fresh = plan.arrival(stage)
    deep = parts * SUB

    def chunk_of(slot):
        k = slot // here
        return chunks[k].at[0] if k < 2 else chunks[k // 2 + 1].at[k % 2]

    def line_of(slot):
        at = plan.data_rows + slot % here
        return chunk_of(slot)[at : at + 1, :]

    per_word = 8
    words = []
    if parts > 1:
        for at in range(0, first_slot, per_word):
            word = before[1][first_slot, 0:1, :][0, at // per_word].astype(jnp.int32)
            words.append(word)
            for u in range(at, min(at + per_word, first_slot)):
                starts[u] = SUB + ((word >> (3 * (u - at))) & 7)
    for i in range(fresh):
        slot = first_slot + i
        line = line_of(slot)
        bits = line[0, n].astype(jnp.int32)
        count = bits % COUNTS
        bits = bits // COUNTS
        for h in range(1, plan.halves):
            bits = bits | (line[0, n + h].astype(jnp.int32) << (16 * h))
        filled = jnp.minimum((count + g - 1) // g, rows)
        starts[slot] = filled
        if parts > 1:
            if slot % per_word == 0:
                words.append(jnp.int32(0))
            more = jnp.maximum(filled - SUB, 0)
            words[-1] = words[-1] + (more << (3 * (slot % per_word)))
        step = 1
        while step < plan.slots:
            low = sum(1 << b for b in range(plan.slots) if not b & step)
            low = low - (1 << 32) if low >= 1 << 31 else low
            turned = ((bits & low) << step) | ((bits >> step) & low)
            bits = jnp.where((me * here) & step != 0, turned, bits)
            step *= 2
        links[i] = bits & ((1 << (first_slot + i)) - 1)

    sphere = iota((rows, LANES), 0) * g + iota((rows, LANES), 1) // width
    last = iota((rows, LANES), 1) % W == W - 1
    for i in range(fresh):
        slot = first_slot + i
        chunk = chunk_of(slot)
        at = slot % here * plan.fields * rows
        fields = [chunk[at + f * rows : at + (f + 1) * rows, :] for f in range(plan.fields)]
        if plan.sweep_late:
            line = line_of(slot)
            wide = jnp.broadcast_to(line, (SUB, LANES))
            pick = iota((SUB, LANES), 0) * g + iota((SUB, LANES), 1) // width
            radius = [
                jnp.take_along_axis(
                    wide, jnp.minimum(pick + p * SUB * g, LANES - 1), axis=1,
                    mode="promise_in_bounds",
                )
                for p in range(parts)
            ]
            fields, swept = sweep(fields, last, jnp.concatenate(radius, axis=0)[:rows])
            count = line[:, n : n + 1].astype(jnp.int32) % COUNTS
            off = FAR * (1 + sphere + plan.padded * slot).astype(jnp.float32)
            fields[0] = jnp.where(sphere < count, fields[0], off)
            fields.append(swept)
        for c in range(4):
            x = fields[c]
            for m in range(1, g):
                blocks[i, c, m, 0:rows, :] = pltpu.roll(x, m * width, 1)
            store[slot, c, 0:rows, :] = x
            if deep > rows:
                fill = jnp.full((deep - rows, LANES), -FAR if c == 0 else 1.0, jnp.float32)
                store[slot, c, rows:deep, :] = fill
        totals[slot] = jnp.zeros((SUB, LANES), jnp.float32)
    for u in range(first_slot):
        store[u] = before[0][u]
        totals[u] = before[1][u]
    if parts > 1 and not ends:
        lane = iota((SUB, LANES), 1)
        line = jnp.zeros((SUB, LANES), jnp.float32)
        for at, word in enumerate(words):
            line = jnp.where(lane == at, word.astype(jnp.float32), line)
        totals[first_slot + fresh] = line

    def row(i, m, r):
        if m == 0:
            return [store[first_slot + i, c, r : r + 1, :] for c in range(4)]
        return [blocks[i, c, m, r : r + 1, :] for c in range(4)]

    def part(slot, p):
        return [store[slot, c, p * SUB : (p + 1) * SUB, :] for c in range(4)]

    sub = iota((SUB, LANES), 0)
    lane_group = iota((SUB, LANES), 1) // width
    nothing = jnp.zeros((SUB, LANES), jnp.float32)

    def self_terms(u, high):
        total = nothing
        second = part(first_slot + u, 0)
        for d in range(SUB // 2 + 1):
            turned = [pltpu.roll(x, SUB - d, 0) for x in second] if d else second
            low = (sub + d) % SUB
            for m in range(g):
                other = (lane_group + g - m) % g
                if d == 0:
                    if m < 2:
                        continue
                    keep = lane_group >= m
                elif d == 1 and m == 1:
                    keep = jnp.abs((low - sub) * g + lane_group - other) >= 2
                elif 2 * d == SUB:
                    keep = sub < d
                else:
                    keep = None
                first = [blocks[u, c, m, 0:SUB, :] for c in range(4)] if m else second
                total = total + masked(term(first, turned), keep)
        for r in range(SUB, high):
            for p in range(parts):
                if p * SUB > r:
                    continue
                second = part(first_slot + u, p)
                for m in range(g):
                    other = (lane_group + g - m) % g
                    ahead = (r - p * SUB - sub) * g + other - lane_group
                    near = r < (p + 1) * SUB + 1
                    total = total + masked(term(row(u, m, r), second), ahead >= 2 if near else None)
        return total

    def against(u, high, second):
        value = nothing
        for r in range(high):
            for m in range(g):
                value = value + term(row(u, m, r), second)
        return value

    def lowest_bit(bits):
        return 31 - lax.clz(bits & -bits)

    def with_rows(u, high):
        total = self_terms(u, high)

        def take(bits, v, filled):
            rest = bits & (bits - 1)
            after = lowest_bit(rest)
            value = against(u, high, part(v, 0))
            totals[v] = totals[v] + value
            if parts > 1:
                for c, x in enumerate(part(v, 1)):
                    tails[c, pl.ds(filled, SUB), :] = x
                filled = filled + jnp.maximum(starts[v] - SUB, 0)
            return rest, after, filled, value

        def two(state):
            bits, filled, total = state
            bits, v, filled, value = take(bits, lowest_bit(bits), filled)
            bits, v, filled, other = take(bits, lowest_bit(bits), filled)
            return bits, filled, total + (value + other)

        def one(state):
            bits, v, filled, total = state
            bits, v, filled, value = take(bits, v, filled)
            return bits, v, filled, total + value

        bits, filled = links[u], jnp.int32(0)
        if ends:
            bits, filled, total = lax.while_loop(
                lambda state: state[0] & (state[0] - 1) != 0, two, (bits, filled, total)
            )
        state = (bits, lowest_bit(bits), filled, total)
        _, _, filled, total = lax.while_loop(lambda state: state[0] != 0, one, state)
        if parts > 1:
            for c in range(4):
                fill = jnp.full((SUB, LANES), -FAR if c == 0 else 1.0, jnp.float32)
                tails[c, pl.ds(filled, SUB), :] = fill

            def trip(j, total):
                at = pl.multiple_of(j * SUB, SUB)
                value = against(u, high, [tails[c, pl.ds(at, SUB), :] for c in range(4)])
                sums[pl.ds(at, SUB), :] = value
                return total + value

            total = lax.fori_loop(0, (filled + SUB - 1) // SUB, trip, total)
        totals[first_slot + u] = totals[first_slot + u] + total

    lowest = max(1, -(-(n // 2) // g))

    def choose(u, low, high):
        if low == high:
            with_rows(u, high)
            return
        middle = (low + high) // 2

        @pl.when(starts[first_slot + u] <= middle)
        def _():
            choose(u, low, middle)

        @pl.when(starts[first_slot + u] > middle)
        def _():
            choose(u, middle + 1, high)

    @pl.loop(0, fresh)
    def _(u):
        choose(u, lowest, rows)
        if parts > 1:

            def hand_out(state):
                bits, v, filled = state
                rest = bits & (bits - 1)
                after = lowest_bit(rest)
                more = jnp.maximum(starts[v] - SUB, 0)
                totals[v] = totals[v] + jnp.where(sub < more, sums[pl.ds(filled, SUB), :], 0.0)
                return rest, after, filled + more

            state = (links[u], lowest_bit(links[u]), jnp.int32(0))
            lax.while_loop(lambda state: state[0] != 0, hand_out, state)

    if not ends:
        return
    spot = iota((1, LANES), 1) // width == me % g
    for k in range(plan.group):
        for l in range(here):
            value = jnp.sum(totals[k * here + l], axis=0, keepdims=True)
            value = sum([pltpu.roll(value, m * width, 1) for m in range(1, g)], value)
            value = jnp.where(spot, value, 0.0) / (n * n)
            out[pl.ds((me ^ k) * here + l, 1), :] = value


def cost(plan, stage, chunks, before):
    first_slot, fresh = plan.arrival(stage)
    slots, g = first_slot + fresh, plan.lane_groups
    deep = plan.parts * SUB
    long = round_up(slots * max(plan.rows - SUB, 0) + 2 * SUB, SUB)
    carried = [(slots, 4, deep, LANES), (slots + 1, SUB, LANES)]
    ends = stage == plan.chips
    outs = [(slots, LANES)] if ends else carried
    scratch = (carried if ends else []) + [(fresh, 4, g, deep, LANES), (4, long, LANES), (long, LANES)]
    return pl.pallas_call(
        functools.partial(cost_kernel, plan, stage),
        out_shape=[jax.ShapeDtypeStruct(shape, jnp.float32) for shape in outs],
        in_specs=[VMEM] * (len(chunks) + len(before)),
        out_specs=[VMEM] * len(outs),
        scratch_shapes=[pltpu.VMEM(shape, jnp.float32) for shape in scratch]
        + [pltpu.SMEM((slots,), jnp.int32), pltpu.SMEM((fresh,), jnp.int32)],
        compiler_params=PARAMS,
        cost_estimate=pl.CostEstimate(
            flops=10_000_000 * (stage + 1), bytes_accessed=1000, transcendentals=0
        ),
        name=f"cost{stage}",
    )(*chunks, *before)


def owner_kernel(plan, costs, out):
    for l in range(plan.here):
        for t in range(plan.tiles):
            out[l : l + 1, t * LANES : (t + 1) * LANES] = owned(plan, costs, l, t)


def owned(plan, costs, l, t):
    here, g = plan.here, plan.lane_groups
    line = costs[t * g * here + l : t * g * here + l + 1, :]
    for d in range(t * g + 1, (t + 1) * g):
        line = line + costs[d * here + l : d * here + l + 1, :]
    return line


def owner(plan, costs):
    return pl.pallas_call(
        functools.partial(owner_kernel, plan),
        out_shape=jax.ShapeDtypeStruct((plan.here, plan.columns), jnp.float32),
        in_specs=[VMEM],
        out_specs=VMEM,
        compiler_params=PARAMS,
        cost_estimate=pl.CostEstimate(flops=4_000_000, bytes_accessed=1000, transcendentals=0),
        name="owner",
    )(costs)


def blend_kernel(plan, seeds_here, costs, stored, sums):
    n, here = plan.spheres, plan.here
    n_rows = n // 4
    step = plan.tiles * here
    seed_of = iota((seeds_here, LANES), 1) // W
    seed = iota((seeds_here, LANES), 0)
    fold = iota((n_rows, LANES), 1) // W
    per_tile = LANES // W
    for l in range(here):
        seed_cost = jnp.zeros((seeds_here, 1), jnp.float32)
        for t in range(plan.tiles):
            line = owned(plan, costs, l, t)
            mine = seed_of + t * per_tile == seed
            seed_cost = seed_cost + jnp.sum(jnp.where(mine, line, 0.0), axis=1, keepdims=True)
        weight = 1.0 / (1.0 + seed_cost)
        spread = []
        for t in range(plan.tiles):
            mine = seed_of + t * per_tile == seed
            spread.append(jnp.sum(jnp.where(mine, weight, 0.0), axis=0, keepdims=True))
        total = jnp.sum(weight, axis=0, keepdims=True)
        sums[here * 3 * n_rows + l : here * 3 * n_rows + l + 1, :] = jnp.broadcast_to(total, (1, LANES))
        for c in range(3):
            pieces = []
            for j in range(4):
                x = jnp.zeros((n_rows, LANES), jnp.float32)
                for t in range(plan.tiles):
                    at = (c * n + j) * step + t * here + l
                    x = x + stored[pl.ds(at, n_rows, stride=4 * step), :] * spread[t]
                pieces.append(x)
            y = jnp.zeros((n_rows, LANES), jnp.float32)
            for turn in range(4):
                z = pieces[0]
                for j in range(4):
                    z = jnp.where(fold == (j - turn) % 4, pieces[j], z)
                y = y + (pltpu.roll(z, turn * W, 1) if turn else z)
            at = (l * 3 + c) * n_rows
            sums[at : at + n_rows, :] = y


def blend(plan, costs, stored):
    seeds_here = plan.columns // W
    rows = round_up(plan.here * (3 * plan.spheres // 4 + 1), SUB)
    return pl.pallas_call(
        functools.partial(blend_kernel, plan, seeds_here),
        out_shape=jax.ShapeDtypeStruct((rows, LANES), jnp.float32),
        in_specs=[VMEM, VMEM],
        out_specs=VMEM,
        compiler_params=PARAMS,
        name="blend",
    )(costs, stored)


def finish_kernel(plan, *refs):
    parts, out, wide = refs[:-2], refs[-2], refs[-1]
    n_rows = plan.spheres // 4
    for l in range(plan.here):
        at = plan.here * 3 * n_rows + l
        total = parts[0][at : at + 1, :]
        for p in parts[1:]:
            total = total + p[at : at + 1, :]
        inverse = 1.0 / total
        for c in range(3):
            at = (l * 3 + c) * n_rows
            y = parts[0][at : at + n_rows, :]
            for p in parts[1:]:
                y = y + p[at : at + n_rows, :]
            y = y * inverse
            for j in range(4):
                z = pltpu.roll(y, (LANES - j * W) % LANES, 1) if j else y
                wide[l * 3 + c, pl.ds(j, n_rows, stride=4), :] = z
            out[l, c] = wide[l * 3 + c].T[:W]


def finish(plan, parts):
    return pl.pallas_call(
        functools.partial(finish_kernel, plan),
        out_shape=jax.ShapeDtypeStruct((plan.here, 3, W, plan.spheres), jnp.float32),
        in_specs=[VMEM] * len(parts),
        out_specs=VMEM,
        scratch_shapes=[pltpu.VMEM((plan.here * 3, plan.spheres, LANES), jnp.float32)],
        compiler_params=PARAMS,
        name="finish",
    )(*parts)


def exchanged(block, axis, k):
    size = lax.axis_size(axis)
    return lax.ppermute(block, axis, [(i, i ^ k) for i in range(size)])


def local(centres, sphere_radius, counts, adjacency):
    here, _, spheres, columns = centres.shape
    plan = Plan(lax.axis_size("robot"), here, spheres, columns)
    stored = centres.reshape(here, 3, spheres, plan.tiles, LANES)
    stored = stored.transpose(1, 2, 3, 0, 4).reshape(-1, LANES)
    theirs, stored, lines = pack(plan, 1, stored, counts.reshape(1, -1), sphere_radius, adjacency)
    theirs = exchanged(theirs, "robot", 1)
    (mine,) = pack(plan, 0, lines, stored)
    carried = cost(plan, 0, [mine], [])
    mine, *carried = lax.optimization_barrier((mine, *carried))
    chunks = [mine, theirs]
    for k, pair in enumerate(join(plan, mine, theirs), 1):
        chunks.append(exchanged(pair, "robot", 2 * k))
    for stage in range(1, plan.chips + 1):
        carried = cost(plan, stage, chunks[: stage + 1], carried)
    (costs,) = carried
    costs = lax.all_to_all(costs, "robot", 0, 0, tiled=True)
    sums = blend(plan, costs, stored)
    parts = [sums] + [exchanged(sums, "seed", k) for k in range(1, lax.axis_size("seed"))]
    return owner(plan, costs), finish(plan, parts).transpose(0, 1, 3, 2)


def solution(mesh):
    return jax.shard_map(
        local,
        mesh=mesh,
        in_specs=(P("robot", None, None, "seed"), P("robot", None), P("robot"), P("robot", None)),
        out_specs=(P("robot", "seed"), P("robot", None, None, None)),
        check_vma=False,
    )
```

```python
import functools
import math

import jax
import jax.numpy as jnp
from jax import lax
from jax.experimental import pallas as pl
from jax.experimental.pallas import tpu as pltpu
from jax.sharding import PartitionSpec as P

W = 32
LANES = 128
SUB = 8
SCALE = math.sqrt(math.log2(math.e))
FAR = 1e15
COUNTS = 64
VMEM = pl.BlockSpec(memory_space=pltpu.VMEM)
SMEM = pl.BlockSpec(memory_space=pltpu.SMEM)
PARAMS = pltpu.CompilerParams(vmem_limit_bytes=16 * 1024 * 1024)


def round_up(value, step):
    return -(-value // step) * step


class Plan:
    def __init__(self, group, robots_here, spheres, columns):
        self.group = group
        self.chips = group // 2
        self.here = robots_here
        self.spheres = spheres
        self.columns = columns
        self.width = columns // group
        self.lane_groups = LANES // self.width
        self.rows = -(-spheres // self.lane_groups)
        self.padded = self.rows * self.lane_groups
        self.parts = -(-self.rows // SUB)
        self.slots = group * robots_here
        self.halves = -(-self.slots // 16)
        self.sweep_late = self.width % W == 0
        self.fields = 3 if self.sweep_late else 4
        self.data_rows = robots_here * self.fields * self.rows
        self.chunk_rows = round_up(self.data_rows + robots_here, SUB)
        self.tiles = columns // LANES

    def arrival(self, stage):
        k = stage if stage < 2 else 2 * (stage - 1)
        return k * self.here, self.here if stage < 2 else 2 * self.here


def iota(shape, axis):
    return lax.broadcasted_iota(jnp.int32, shape, axis)


def sweep(points, last, radius):
    squares = None
    middles = []
    for x in points:
        ahead = jnp.where(last, x, pltpu.roll(x, LANES - 1, 1))
        middles.append((0.5 * SCALE) * (x + ahead))
        square = (ahead - x) * (ahead - x)
        squares = square if squares is None else squares + square
    return middles, radius + 0.5 * jnp.sqrt(squares + 1e-06)


def fetch(plan, sources, stored, lines, counts, radius, adjacency, sem):
    n = plan.spheres
    copies = [
        pltpu.make_async_copy(src, dst, sem.at[i])
        for i, (src, dst) in enumerate(zip(sources, (stored, counts, radius, adjacency)))
    ]
    for copy in copies:
        copy.start()
    for copy in copies[1:]:
        copy.wait()
    lane = iota((1, LANES), 1)
    links = iota((1, plan.slots), 1)
    for l in range(plan.here):
        head = jnp.zeros((1, LANES), jnp.float32)
        for h in range(plan.halves):
            bits = jnp.where(
                (adjacency[l : l + 1, :] != 0) & (links // 16 == h), 1 << (links % 16), 0
            )
            value = jnp.sum(bits.astype(jnp.float32), axis=1, keepdims=True)
            if h == 0:
                value = value * COUNTS + counts[:, l : l + 1].astype(jnp.float32)
            head = jnp.where(lane == n + h, value, head)
        lines[l : l + 1, :] = head
        lines[l : l + 1, 0:n] = radius[l : l + 1, :]
    copies[0].wait()


def pack_kernel(plan, core, *refs):
    if core:
        out, stored, lines, source = refs[4:8]
        fetch(plan, refs[:4], stored, lines, *refs[8:])
    else:
        lines, stored, out, source = refs
    me = lax.axis_index("robot")
    n, g, rows, width, here = plan.spheres, plan.lane_groups, plan.rows, plan.width, plan.here
    step = plan.tiles * here
    if not plan.sweep_late:
        order = iota((n, LANES), 0)
        diagonal = iota((n, n), 0) == iota((n, n), 1)
        for l in range(here):
            column = jnp.sum(jnp.where(diagonal, lines[l : l + 1, 0:n], 0.0), axis=1, keepdims=True)
            count = lines[l : l + 1, n : n + 1].astype(jnp.int32) % COUNTS
            robot = me * here + l
            off = FAR * (1 + order + plan.padded * robot).astype(jnp.float32)
            for t in range(plan.tiles):
                points = [
                    stored[pl.ds(c * n * step + t * here + l, n, stride=step), :] for c in range(3)
                ]
                fields, swept = sweep(points, iota((n, LANES), 1) % W == W - 1, column)
                fields[0] = jnp.where(order < count, fields[0], off)
                for c, x in enumerate(fields + [swept]):
                    source[t, l * 4 + c, 0:n, :] = x
                if plan.padded > n:
                    index = n + iota((plan.padded - n, LANES), 0) + plan.padded * robot
                    fill = FAR * (1 + index).astype(jnp.float32)
                    for c in range(4):
                        source[t, l * 4 + c, n:, :] = fill if c == 0 else jnp.ones_like(fill)
    lane_group = iota((rows, LANES), 1) // width
    for k in range(plan.chips):
        dest = me ^ (2 * k + core)
        tile = dest // g
        spot = dest % g
        for l in range(here):
            for c in range(plan.fields):
                y = jnp.zeros((rows, LANES), jnp.float32)
                for j in range(g):
                    if plan.sweep_late:
                        at = (c * n + j) * step + tile * here + l
                        x = stored[pl.ds(at, rows, stride=g * step), :]
                    else:
                        x = source[tile, l * 4 + c, pl.ds(j, rows, stride=g), :]
                    x = pltpu.roll(x, ((j + g - spot) % g) * width, 1)
                    y = jnp.where(lane_group == j, x, y)
                at = (l * plan.fields + c) * rows
                out[k, at : at + rows, :] = y
            at = plan.data_rows + l
            out[k, at : at + 1, :] = lines[l : l + 1, :]


def pack(plan, core, *args):
    shapes = [(plan.chips, plan.chunk_rows, LANES)]
    swept = (plan.tiles, plan.here * 4, plan.padded, LANES)
    scratch = [pltpu.VMEM((SUB, LANES) if plan.sweep_late else swept, jnp.float32)]
    specs = [VMEM, VMEM]
    if core:
        shapes += [args[0].shape, (plan.here, LANES)]
        scratch += [pltpu.VMEM(x.shape, x.dtype) for x in args[1:]]
        scratch += [pltpu.SemaphoreType.DMA((len(args),))]
        specs = [pl.BlockSpec(memory_space=pltpu.HBM)] * len(args)
        args = [pltpu.with_memory_space_constraint(x, pltpu.HBM) for x in args]
    return pl.pallas_call(
        functools.partial(pack_kernel, plan, core),
        out_shape=[jax.ShapeDtypeStruct(shape, jnp.float32) for shape in shapes],
        in_specs=specs,
        out_specs=[VMEM] * len(shapes),
        scratch_shapes=scratch,
        compiler_params=PARAMS,
        cost_estimate=pl.CostEstimate(flops=4_000_000, bytes_accessed=1000, transcendentals=0),
        name=f"pack{core}",
    )(*args)


def join_kernel(plan, mine, theirs, *outs):
    for k in range(1, plan.chips):
        outs[k - 1][0] = mine[k]
        outs[k - 1][1] = theirs[k]


def join(plan, mine, theirs):
    pair = jax.ShapeDtypeStruct((2, plan.chunk_rows, LANES), jnp.float32)
    return pl.pallas_call(
        functools.partial(join_kernel, plan),
        out_shape=[pair] * (plan.chips - 1),
        in_specs=[VMEM, VMEM],
        out_specs=[VMEM] * (plan.chips - 1),
        compiler_params=PARAMS,
        name="join",
    )(mine, theirs)


def term(first, second):
    gap = first[0] - second[0]
    square = gap * gap
    for c in (1, 2):
        gap = first[c] - second[c]
        square = square + gap * gap
    inverse = 1.0 / (first[3] + second[3])
    return jnp.exp2(-(square * (inverse * inverse)))


def masked(value, keep):
    return value if keep is None else jnp.where(keep, value, 0.0)


def cost_kernel(plan, stage, *refs):
    chunks, refs = refs[: stage + 1], refs[stage + 1 :]
    before, refs = refs[: 2 if stage else 0], refs[2 if stage else 0 :]
    ends = stage == plan.chips
    if ends:
        out, store, totals, blocks, tails, sums, starts, links = refs
    else:
        store, totals, blocks, tails, sums, starts, links = refs
    me = lax.axis_index("robot")
    g, rows, width, here, n = plan.lane_groups, plan.rows, plan.width, plan.here, plan.spheres
    parts = plan.parts
    first_slot, fresh = plan.arrival(stage)
    deep = parts * SUB

    def chunk_of(slot):
        k = slot // here
        return chunks[k].at[0] if k < 2 else chunks[k // 2 + 1].at[k % 2]

    def line_of(slot):
        at = plan.data_rows + slot % here
        return chunk_of(slot)[at : at + 1, :]

    per_word = 8
    words = []
    if parts > 1:
        for at in range(0, first_slot, per_word):
            word = before[1][first_slot, 0:1, :][0, at // per_word].astype(jnp.int32)
            words.append(word)
            for u in range(at, min(at + per_word, first_slot)):
                starts[u] = SUB + ((word >> (3 * (u - at))) & 7)
    for i in range(fresh):
        slot = first_slot + i
        line = line_of(slot)
        bits = line[0, n].astype(jnp.int32)
        count = bits % COUNTS
        bits = bits // COUNTS
        for h in range(1, plan.halves):
            bits = bits | (line[0, n + h].astype(jnp.int32) << (16 * h))
        filled = jnp.minimum((count + g - 1) // g, rows)
        starts[slot] = filled
        if parts > 1:
            if slot % per_word == 0:
                words.append(jnp.int32(0))
            more = jnp.maximum(filled - SUB, 0)
            words[-1] = words[-1] + (more << (3 * (slot % per_word)))
        step = 1
        while step < plan.slots:
            low = sum(1 << b for b in range(plan.slots) if not b & step)
            low = low - (1 << 32) if low >= 1 << 31 else low
            turned = ((bits & low) << step) | ((bits >> step) & low)
            bits = jnp.where((me * here) & step != 0, turned, bits)
            step *= 2
        links[i] = bits & ((1 << (first_slot + i)) - 1)

    sphere = iota((rows, LANES), 0) * g + iota((rows, LANES), 1) // width
    last = iota((rows, LANES), 1) % W == W - 1
    for i in range(fresh):
        slot = first_slot + i
        chunk = chunk_of(slot)
        at = slot % here * plan.fields * rows
        fields = [chunk[at + f * rows : at + (f + 1) * rows, :] for f in range(plan.fields)]
        if plan.sweep_late:
            line = line_of(slot)
            wide = jnp.broadcast_to(line, (SUB, LANES))
            pick = iota((SUB, LANES), 0) * g + iota((SUB, LANES), 1) // width
            radius = [
                jnp.take_along_axis(
                    wide, jnp.minimum(pick + p * SUB * g, LANES - 1), axis=1,
                    mode="promise_in_bounds",
                )
                for p in range(parts)
            ]
            fields, swept = sweep(fields, last, jnp.concatenate(radius, axis=0)[:rows])
            count = line[:, n : n + 1].astype(jnp.int32) % COUNTS
            off = FAR * (1 + sphere + plan.padded * slot).astype(jnp.float32)
            fields[0] = jnp.where(sphere < count, fields[0], off)
            fields.append(swept)
        for c in range(4):
            x = fields[c]
            for m in range(1, g):
                blocks[i, c, m, 0:rows, :] = pltpu.roll(x, m * width, 1)
                if rows < SUB:
                    fill = jnp.full((SUB - rows, LANES), -2 * FAR if c == 0 else 1.0, jnp.float32)
                    blocks[i, c, m, rows:SUB, :] = fill
            store[slot, c, 0:rows, :] = x
            if deep > rows:
                fill = jnp.full((deep - rows, LANES), -FAR if c == 0 else 1.0, jnp.float32)
                store[slot, c, rows:deep, :] = fill
        totals[slot] = jnp.zeros((SUB, LANES), jnp.float32)
    for u in range(first_slot):
        store[u] = before[0][u]
        totals[u] = before[1][u]
    if parts > 1 and not ends:
        lane = iota((SUB, LANES), 1)
        line = jnp.zeros((SUB, LANES), jnp.float32)
        for at, word in enumerate(words):
            line = jnp.where(lane == at, word.astype(jnp.float32), line)
        totals[first_slot + fresh] = line

    def row(i, m, r):
        if m == 0:
            return [store[first_slot + i, c, r : r + 1, :] for c in range(4)]
        return [blocks[i, c, m, r : r + 1, :] for c in range(4)]

    def part(slot, p):
        return [store[slot, c, p * SUB : (p + 1) * SUB, :] for c in range(4)]

    sub = iota((SUB, LANES), 0)
    lane_group = iota((SUB, LANES), 1) // width
    nothing = jnp.zeros((SUB, LANES), jnp.float32)

    def self_terms(u, high):
        total = nothing
        second = part(first_slot + u, 0)
        for d in range(SUB // 2 + 1):
            turned = [pltpu.roll(x, SUB - d, 0) for x in second] if d else second
            low = (sub + d) % SUB
            for m in range(g):
                other = (lane_group + g - m) % g
                if d == 0:
                    if m < 2:
                        continue
                    keep = lane_group >= m
                elif d == 1 and m == 1:
                    keep = jnp.abs((low - sub) * g + lane_group - other) >= 2
                elif 2 * d == SUB:
                    keep = sub < d
                else:
                    keep = None
                first = [blocks[u, c, m, 0:SUB, :] for c in range(4)] if m else second
                total = total + masked(term(first, turned), keep)
        for r in range(SUB, high):
            for p in range(parts):
                if p * SUB > r:
                    continue
                second = part(first_slot + u, p)
                for m in range(g):
                    other = (lane_group + g - m) % g
                    ahead = (r - p * SUB - sub) * g + other - lane_group
                    near = r < (p + 1) * SUB + 1
                    total = total + masked(term(row(u, m, r), second), ahead >= 2 if near else None)
        return total

    def against(u, high, second):
        value = nothing
        for r in range(high):
            for m in range(g):
                value = value + term(row(u, m, r), second)
        return value

    def lowest_bit(bits):
        return 31 - lax.clz(bits & -bits)

    def with_rows(u, high):
        total = self_terms(u, high)

        def take(bits, v, filled):
            rest = bits & (bits - 1)
            after = lowest_bit(rest)
            value = against(u, high, part(v, 0))
            totals[v] = totals[v] + value
            if parts > 1:
                for c, x in enumerate(part(v, 1)):
                    tails[c, pl.ds(filled, SUB), :] = x
                filled = filled + jnp.maximum(starts[v] - SUB, 0)
            return rest, after, filled, value

        def two(state):
            bits, filled, total = state
            bits, v, filled, value = take(bits, lowest_bit(bits), filled)
            bits, v, filled, other = take(bits, lowest_bit(bits), filled)
            return bits, filled, total + (value + other)

        def one(state):
            bits, v, filled, total = state
            bits, v, filled, value = take(bits, v, filled)
            return bits, v, filled, total + value

        bits, filled = links[u], jnp.int32(0)
        if ends:
            bits, filled, total = lax.while_loop(
                lambda state: state[0] & (state[0] - 1) != 0, two, (bits, filled, total)
            )
        state = (bits, lowest_bit(bits), filled, total)
        _, _, filled, total = lax.while_loop(lambda state: state[0] != 0, one, state)
        if parts > 1:
            for c in range(4):
                fill = jnp.full((SUB, LANES), -FAR if c == 0 else 1.0, jnp.float32)
                tails[c, pl.ds(filled, SUB), :] = fill

            def trip(j, total):
                at = pl.multiple_of(j * SUB, SUB)
                value = against(u, high, [tails[c, pl.ds(at, SUB), :] for c in range(4)])
                sums[pl.ds(at, SUB), :] = value
                return total + value

            total = lax.fori_loop(0, (filled + SUB - 1) // SUB, trip, total)
        totals[first_slot + u] = totals[first_slot + u] + total

    lowest = max(1, -(-(n // 2) // g))

    def choose(u, low, high):
        if low == high:
            with_rows(u, high)
            return
        middle = (low + high) // 2

        @pl.when(starts[first_slot + u] <= middle)
        def _():
            choose(u, low, middle)

        @pl.when(starts[first_slot + u] > middle)
        def _():
            choose(u, middle + 1, high)

    @pl.loop(0, fresh)
    def _(u):
        choose(u, lowest, rows)
        if parts > 1:

            def hand_out(state):
                bits, v, filled = state
                rest = bits & (bits - 1)
                after = lowest_bit(rest)
                more = jnp.maximum(starts[v] - SUB, 0)
                totals[v] = totals[v] + jnp.where(sub < more, sums[pl.ds(filled, SUB), :], 0.0)
                return rest, after, filled + more

            state = (links[u], lowest_bit(links[u]), jnp.int32(0))
            lax.while_loop(lambda state: state[0] != 0, hand_out, state)

    if not ends:
        return
    spot = iota((1, LANES), 1) // width == me % g
    for k in range(plan.group):
        for l in range(here):
            value = jnp.sum(totals[k * here + l], axis=0, keepdims=True)
            value = sum([pltpu.roll(value, m * width, 1) for m in range(1, g)], value)
            value = jnp.where(spot, value, 0.0) / (n * n)
            out[pl.ds((me ^ k) * here + l, 1), :] = value


def cost(plan, stage, chunks, before):
    first_slot, fresh = plan.arrival(stage)
    slots, g = first_slot + fresh, plan.lane_groups
    deep = plan.parts * SUB
    long = round_up(slots * max(plan.rows - SUB, 0) + 2 * SUB, SUB)
    carried = [(slots, 4, deep, LANES), (slots + 1, SUB, LANES)]
    ends = stage == plan.chips
    outs = [(slots, LANES)] if ends else carried
    scratch = (carried if ends else []) + [(fresh, 4, g, deep, LANES), (4, long, LANES), (long, LANES)]
    return pl.pallas_call(
        functools.partial(cost_kernel, plan, stage),
        out_shape=[jax.ShapeDtypeStruct(shape, jnp.float32) for shape in outs],
        in_specs=[VMEM] * (len(chunks) + len(before)),
        out_specs=[VMEM] * len(outs),
        scratch_shapes=[pltpu.VMEM(shape, jnp.float32) for shape in scratch]
        + [pltpu.SMEM((slots,), jnp.int32), pltpu.SMEM((fresh,), jnp.int32)],
        compiler_params=PARAMS,
        cost_estimate=pl.CostEstimate(
            flops=10_000_000 * (stage + 1), bytes_accessed=1000, transcendentals=0
        ),
        name=f"cost{stage}",
    )(*chunks, *before)


def owner_kernel(plan, costs, out):
    for l in range(plan.here):
        for t in range(plan.tiles):
            out[l : l + 1, t * LANES : (t + 1) * LANES] = owned(plan, costs, l, t)


def owned(plan, costs, l, t):
    here, g = plan.here, plan.lane_groups
    line = costs[t * g * here + l : t * g * here + l + 1, :]
    for d in range(t * g + 1, (t + 1) * g):
        line = line + costs[d * here + l : d * here + l + 1, :]
    return line


def owner(plan, costs):
    return pl.pallas_call(
        functools.partial(owner_kernel, plan),
        out_shape=jax.ShapeDtypeStruct((plan.here, plan.columns), jnp.float32),
        in_specs=[VMEM],
        out_specs=VMEM,
        compiler_params=PARAMS,
        cost_estimate=pl.CostEstimate(flops=4_000_000, bytes_accessed=1000, transcendentals=0),
        name="owner",
    )(costs)


def blend_kernel(plan, seeds_here, costs, stored, sums):
    n, here = plan.spheres, plan.here
    n_rows = n // 4
    step = plan.tiles * here
    seed_of = iota((seeds_here, LANES), 1) // W
    seed = iota((seeds_here, LANES), 0)
    fold = iota((n_rows, LANES), 1) // W
    per_tile = LANES // W
    for l in range(here):
        seed_cost = jnp.zeros((seeds_here, 1), jnp.float32)
        for t in range(plan.tiles):
            line = owned(plan, costs, l, t)
            mine = seed_of + t * per_tile == seed
            seed_cost = seed_cost + jnp.sum(jnp.where(mine, line, 0.0), axis=1, keepdims=True)
        weight = 1.0 / (1.0 + seed_cost)
        spread = []
        for t in range(plan.tiles):
            mine = seed_of + t * per_tile == seed
            spread.append(jnp.sum(jnp.where(mine, weight, 0.0), axis=0, keepdims=True))
        total = jnp.sum(weight, axis=0, keepdims=True)
        sums[here * 3 * n_rows + l : here * 3 * n_rows + l + 1, :] = jnp.broadcast_to(total, (1, LANES))
        for c in range(3):
            pieces = []
            for j in range(4):
                x = jnp.zeros((n_rows, LANES), jnp.float32)
                for t in range(plan.tiles):
                    at = (c * n + j) * step + t * here + l
                    x = x + stored[pl.ds(at, n_rows, stride=4 * step), :] * spread[t]
                pieces.append(x)
            y = jnp.zeros((n_rows, LANES), jnp.float32)
            for turn in range(4):
                z = pieces[0]
                for j in range(4):
                    z = jnp.where(fold == (j - turn) % 4, pieces[j], z)
                y = y + (pltpu.roll(z, turn * W, 1) if turn else z)
            at = (l * 3 + c) * n_rows
            sums[at : at + n_rows, :] = y


def blend(plan, costs, stored):
    seeds_here = plan.columns // W
    rows = round_up(plan.here * (3 * plan.spheres // 4 + 1), SUB)
    return pl.pallas_call(
        functools.partial(blend_kernel, plan, seeds_here),
        out_shape=jax.ShapeDtypeStruct((rows, LANES), jnp.float32),
        in_specs=[VMEM, VMEM],
        out_specs=VMEM,
        compiler_params=PARAMS,
        name="blend",
    )(costs, stored)


def finish_kernel(plan, *refs):
    parts, out, wide = refs[:-2], refs[-2], refs[-1]
    n_rows = plan.spheres // 4
    for l in range(plan.here):
        at = plan.here * 3 * n_rows + l
        total = parts[0][at : at + 1, :]
        for p in parts[1:]:
            total = total + p[at : at + 1, :]
        inverse = 1.0 / total
        for c in range(3):
            at = (l * 3 + c) * n_rows
            y = parts[0][at : at + n_rows, :]
            for p in parts[1:]:
                y = y + p[at : at + n_rows, :]
            y = y * inverse
            for j in range(4):
                z = pltpu.roll(y, (LANES - j * W) % LANES, 1) if j else y
                wide[l * 3 + c, pl.ds(j, n_rows, stride=4), :] = z
            out[l, c] = wide[l * 3 + c].T[:W]


def finish(plan, parts):
    return pl.pallas_call(
        functools.partial(finish_kernel, plan),
        out_shape=jax.ShapeDtypeStruct((plan.here, 3, W, plan.spheres), jnp.float32),
        in_specs=[VMEM] * len(parts),
        out_specs=VMEM,
        scratch_shapes=[pltpu.VMEM((plan.here * 3, plan.spheres, LANES), jnp.float32)],
        compiler_params=PARAMS,
        name="finish",
    )(*parts)


def exchanged(block, axis, k):
    size = lax.axis_size(axis)
    return lax.ppermute(block, axis, [(i, i ^ k) for i in range(size)])


def local(centres, sphere_radius, counts, adjacency):
    here, _, spheres, columns = centres.shape
    plan = Plan(lax.axis_size("robot"), here, spheres, columns)
    stored = centres.reshape(here, 3, spheres, plan.tiles, LANES)
    stored = stored.transpose(1, 2, 3, 0, 4).reshape(-1, LANES)
    theirs, stored, lines = pack(plan, 1, stored, counts.reshape(1, -1), sphere_radius, adjacency)
    theirs = exchanged(theirs, "robot", 1)
    (mine,) = pack(plan, 0, lines, stored)
    carried = cost(plan, 0, [mine], [])
    mine, *carried = lax.optimization_barrier((mine, *carried))
    chunks = [mine, theirs]
    for k, pair in enumerate(join(plan, mine, theirs), 1):
        chunks.append(exchanged(pair, "robot", 2 * k))
    for stage in range(1, plan.chips + 1):
        carried = cost(plan, stage, chunks[: stage + 1], carried)
    (costs,) = carried
    costs = lax.all_to_all(costs, "robot", 0, 0, tiled=True)
    sums = blend(plan, costs, stored)
    parts = [sums] + [exchanged(sums, "seed", k) for k in range(1, lax.axis_size("seed"))]
    return owner(plan, costs), finish(plan, parts).transpose(0, 1, 3, 2)


def solution(mesh):
    return jax.shard_map(
        local,
        mesh=mesh,
        in_specs=(P("robot", None, None, "seed"), P("robot", None), P("robot"), P("robot", None)),
        out_specs=(P("robot", "seed"), P("robot", None, None, None)),
        check_vma=False,
    )
```
